32 devices in a mesh: parts: 1 (over z), data: 32 (over y, x, core).
Axes of the slice: x: 4, y: 4, z: 1, core: 2. Of those that a mesh axis runs over, the one named last changes fastest.
The devices are a block of a 4x4x8 slice.
Arguments:
- feats: bfloat16 [32768, 784], P('data')
- labels: int32 [32768], P('data')
- w_in: float32 [784, 2, 400], P(None, 'parts')
- w_out: float32 [2, 400], P('parts')
- mom_in: float32 [784, 2, 400], P(None, 'parts')
- mom_out: float32 [2, 400], P('parts')
Outputs:
- output 1: float32 [784, 2, 400], P(None, 'parts')
- output 2: float32 [2, 400], P('parts')
- output 3: float32 [784, 2, 400], P(None, 'parts')
- output 4: float32 [2, 400], P('parts')
- output 5: float32 [2], P('parts')
All inputs are finite; a program needn't handle non-finite values.
Results may differ from the reference program's by a relative error of at most 0.001.
Values are sent between devices in bfloat16 or wider.
A program may use at most 768 MiB of HBM per device.

```python
import math
import jax
import jax.numpy as jnp
from jax import lax

D = 784
HIDDEN = 400
CHAINS = 2
ROWS_DEV = 1024
GROUP = 32
LEAPS = 16
N_ROWS = ROWS_DEV * GROUP
STEP = 1.0 / math.sqrt(N_ROWS * (D + HIDDEN))
PRIOR_VAR = 1.0


def setup_inputs(seed: int = 0, part: int = 0) -> dict:
    key = jax.random.key(seed)
    key_mean, key_noise, key_rate, key_draw, key_part = jax.random.split(key, 5)
    centers = jax.random.normal(key_mean, (GROUP, 1, D), jnp.float32)
    noise = jax.random.normal(key_noise, (GROUP, ROWS_DEV, D), jnp.float32)
    feats = (centers + noise).reshape(N_ROWS, D).astype(jnp.bfloat16)
    rates = jax.random.randint(key_rate, (GROUP, 1), 50, 951)
    draws = jax.random.randint(key_draw, (GROUP, ROWS_DEV), 0, 1000)
    labels = (draws < rates).astype(jnp.int32).reshape(N_ROWS)
    part_key = jax.random.fold_in(key_part, part)
    key_w1, key_w2, key_m1, key_m2 = jax.random.split(part_key, 4)
    w_in = jax.random.normal(key_w1, (D, CHAINS, HIDDEN), jnp.float32) * (2.0 * D) ** -0.5
    w_out = jax.random.normal(key_w2, (CHAINS, HIDDEN), jnp.float32) * (1.5 * HIDDEN ** -0.5)
    mom_in = jax.random.normal(key_m1, (D, CHAINS, HIDDEN), jnp.float32)
    mom_out = jax.random.normal(key_m2, (CHAINS, HIDDEN), jnp.float32)
    return {'feats': feats, 'labels': labels, 'w_in': w_in, 'w_out': w_out, 'mom_in': mom_in, 'mom_out': mom_out}


def block_terms(x_rows, lab_rows, w_flat, w_out):
    pre_act = jnp.dot(x_rows, w_flat, preferred_element_type=jnp.float32).reshape(ROWS_DEV, CHAINS, HIDDEN)
    hidden_act = jnp.tanh(pre_act)
    logits = jnp.sum(hidden_act * w_out, axis=-1)
    residual = lab_rows[:, None] - jax.nn.sigmoid(logits)
    grad_out = jnp.sum(hidden_act * residual[:, :, None], axis=0)
    back_grad = (residual[:, :, None] * w_out * (1.0 - hidden_act * hidden_act)).astype(jnp.bfloat16)
    grad_in = jnp.dot(x_rows.T, back_grad.reshape(ROWS_DEV, CHAINS * HIDDEN), preferred_element_type=jnp.float32)
    return grad_in.reshape(D, CHAINS, HIDDEN), grad_out, logits


def log_post_grad(x_blocks, lab_blocks, w_in, w_out):
    w_flat = w_in.astype(jnp.bfloat16).reshape(D, CHAINS * HIDDEN)

    def row_block(acc_sum, block_in):
        grad_in, grad_out, logits = block_terms(block_in[0], block_in[1], w_flat, w_out)
        return (acc_sum[0] + grad_in, acc_sum[1] + grad_out), logits

    sums, logits = lax.scan(row_block, (jnp.zeros_like(w_in), jnp.zeros_like(w_out)), (x_blocks, lab_blocks))
    return sums[0] - w_in / PRIOR_VAR, sums[1] - w_out / PRIOR_VAR, logits


def reference(feats, labels, w_in, w_out, mom_in, mom_out):
    x_blocks = feats.reshape(GROUP, ROWS_DEV, D)
    lab_blocks = labels.astype(jnp.float32).reshape(GROUP, ROWS_DEV)
    grad_in, grad_out, logits = log_post_grad(x_blocks, lab_blocks, w_in, w_out)
    mom_in = mom_in + 0.5 * STEP * grad_in
    mom_out = mom_out + 0.5 * STEP * grad_out

    def leap_step(state_now, unused):
        pos_in, pos_out, vel_in, vel_out = state_now
        pos_in = pos_in + STEP * vel_in
        pos_out = pos_out + STEP * vel_out
        g_in, g_out, g_logits = log_post_grad(x_blocks, lab_blocks, pos_in, pos_out)
        return (pos_in, pos_out, vel_in + STEP * g_in, vel_out + STEP * g_out), None

    state_end, unused_out = lax.scan(leap_step, (w_in, w_out, mom_in, mom_out), None, length=LEAPS - 1)
    pos_in, pos_out, vel_in, vel_out = state_end
    pos_in = pos_in + STEP * vel_in
    pos_out = pos_out + STEP * vel_out
    grad_in, grad_out, logits = log_post_grad(x_blocks, lab_blocks, pos_in, pos_out)
    vel_in = vel_in + 0.5 * STEP * grad_in
    vel_out = vel_out + 0.5 * STEP * grad_out
    row_loss = jnp.sum(jax.nn.softplus(logits) - lab_blocks[:, :, None] * logits, axis=(0, 1))
    energy = row_loss + (jnp.sum(pos_in * pos_in, axis=(0, 2)) + jnp.sum(pos_out * pos_out, axis=1)) / (2.0 * PRIOR_VAR) + 0.5 * (jnp.sum(vel_in * vel_in, axis=(0, 2)) + jnp.sum(vel_out * vel_out, axis=1))
    return pos_in, pos_out, vel_in, vel_out, energy
```

```python
import functools
import math

import jax
import jax.numpy as jnp
from jax import lax
from jax.experimental import pallas as pl
from jax.experimental.pallas import tpu as pltpu
from jax.sharding import PartitionSpec as P

LEAPS = 16
PRIOR_VAR = 1.0
LANE = 128
PACK = 16
MESH_ID = pl.DeviceIdType.MESH


def _kernel(cfg, xt_hbm, lab_ref, w_hbm, m_hbm, wo_ref, mo_ref, fin_w, fin_m, misc_ref,
            xt, x, ybuf, wload, wb, abuf, bbuf, gacc, g2acc, gsend, rsbuf, pos, mom, w2b, m2b, w2z, wag, zbuf, ztot,
            fin, obuf, lsem, isend, irecv, ysend, yrecv, zsend, zrecv, rsend, rrecv, asend, arecv, fsend, frecv, osem):
    side, hidden, feat, rows, hs, step = cfg
    half = side // 2
    nshard = 2 * side
    nfull = feat // LANE
    rem = feat - nfull * LANE
    nrow = hs // PACK
    nunit = nrow * nfull + 1
    own = -(-nunit // side)
    urows = own * PACK
    kpad = xt.shape[0]
    nlt = rows // LANE
    groups = zsend.shape[1]
    per_group = nshard // groups
    f32, bf16 = jnp.float32, jnp.bfloat16

    me = lax.axis_index('data')
    core = me % 2
    xx = (me // 2) % side
    yy = me // (2 * side)

    def fold(y, x_):
        return (x_ // half + y // half) % 2

    q = (core + fold(yy, xx)) % 2
    zpos = xx * (1 - q) + yy * q
    rpos = yy * (1 - q) + xx * q

    def device(z, r, role):
        x2 = z * (1 - role) + r * role
        y2 = r * (1 - role) + z * role
        return {'data': (y2 * side + x2) * 2 + (role + fold(y2, x2)) % 2}

    zpeer = [device((zpos + d) % side, rpos, q) for d in range(side)]
    rpeer = [device(zpos, (rpos + d) % side, q) for d in range(side)]
    partner = device(rpos, zpos, 1 - q)

    def remote(src, dst, ssem, rsem, dev):
        return pltpu.make_async_remote_copy(src_ref=src, dst_ref=dst, send_sem=ssem, recv_sem=rsem,
                                            device_id=dev, device_id_type=MESH_ID)

    start = jnp.minimum(zpos * hs, hidden - hs)
    start = pl.multiple_of(start, 8)
    cut = zpos * hs - start

    own_slot = 2 * zpos + q
    par_slot = 2 * zpos + (1 - q)

    def xcols(slot):
        return xt.at[pl.ds(0, feat), pl.ds(pl.multiple_of(slot * rows, rows), rows)]

    load_x = pltpu.make_async_copy(xt_hbm, xcols(own_slot), lsem.at[0])
    load_w = pltpu.make_async_copy(w_hbm.at[q, pl.ds(start, hs), :], wload.at[0], lsem.at[1])
    load_m = pltpu.make_async_copy(m_hbm.at[q, pl.ds(start, hs), :], wload.at[1], lsem.at[2])
    load_x.start()
    load_w.start()
    load_m.start()

    barrier = pltpu.get_barrier_semaphore()
    for dev in zpeer[1:] + rpeer[1:] + [partner]:
        pl.semaphore_signal(barrier, inc=1, device_id=dev, device_id_type=MESH_ID)
    pl.semaphore_wait(barrier, 2 * side - 1)

    def ship(i, slot, dslot, dev):
        cx = remote(xcols(slot), xcols(dslot), isend.at[i], irecv.at[i], dev)
        cy = remote(ybuf.at[slot], ybuf.at[dslot], ysend.at[i], yrecv.at[i], dev)
        cx.start()
        cy.start()
        return cx, cy

    def landed(pair):
        pair[0].wait_recv()
        pair[1].wait_recv()

    def turn(slot):
        def body(t, _):
            off = pl.multiple_of(slot * rows + t * LANE, LANE)
            x[pl.ds(off, LANE), :] = xt[:, pl.ds(off, LANE)].T
            return 0
        lax.fori_loop(0, rows // LANE, body, 0)

    ybuf[own_slot] = lab_ref[...]
    xt[pl.ds(feat, kpad - feat), :] = jnp.zeros((kpad - feat, nshard * rows), bf16)
    load_x.wait()
    up, down, far = (zpos + 1) % side, (zpos + side - 1) % side, (zpos + 2) % side
    s0 = ship(0, own_slot, 2 * rpos + q, partner)
    s1 = ship(1, own_slot, own_slot, zpeer[1])
    s4 = ship(4, own_slot, own_slot, zpeer[side - 1])
    turn(own_slot)

    lane = lax.broadcasted_iota(jnp.int32, (PACK, LANE), 1)
    lane8 = lax.broadcasted_iota(jnp.int32, (8, LANE), 1)
    sub8 = lax.broadcasted_iota(jnp.int32, (8, LANE), 0)

    def unit_at(u):
        return u // own, (u % own) * PACK

    def pack(src, dst, width):
        for i in range(nrow):
            for k in range(nfull):
                o, j = unit_at(i * nfull + k)
                dst[o, j:j + PACK, :] = src[i * PACK:(i + 1) * PACK, k * LANE:(k + 1) * LANE]
        o, j = unit_at(nunit - 1)
        acc = jnp.zeros((PACK, LANE), f32)
        for i in range(nrow):
            v = src[i * PACK:(i + 1) * PACK, nfull * LANE:nfull * LANE + width]
            if width < LANE:
                v = jnp.concatenate([v, jnp.zeros((PACK, LANE - width), f32)], axis=1)
            acc = acc + (pltpu.roll(v, i * rem, 1) if i else v)
        dst[o, j:j + PACK, :] = acc

    for o in range(side):
        for u in range(nunit, side * own):
            if u // own == o:
                gsend[o, (u % own) * PACK:(u % own + 1) * PACK, :] = jnp.zeros((PACK, LANE), f32)
    load_w.wait()
    load_m.wait()
    pack(wload.at[1], gsend, rem)
    mom[...] = gsend[rpos, 0:urows, :]
    pack(wload.at[0], gsend, rem)
    pos[...] = gsend[rpos, 0:urows, :]
    wb[:, nfull * LANE:] = jnp.zeros((hs, kpad - nfull * LANE), bf16)
    wb[:, 0:feat] = wload[0].astype(bf16)

    def column(ref, dst):
        width = -(-hidden // LANE) * LANE
        v = jnp.concatenate([ref[pl.ds(q, 1), :], jnp.zeros((1, width - hidden), f32)], axis=1)
        lanes = lax.broadcasted_iota(jnp.int32, (8, width), 1)
        subs = lax.broadcasted_iota(jnp.int32, (8, width), 0)
        v = jnp.broadcast_to(v, (8, width))
        for i in range(hs // 8):
            hit = jnp.where(lanes == start + i * 8 + subs, v, 0.0)
            dst[i * 8:(i + 1) * 8, :] = jnp.broadcast_to(jnp.sum(hit, axis=1, keepdims=True), (8, LANE))

    column(wo_ref, w2b)
    column(mo_ref, m2b)

    landed(s0)
    s2 = ship(2, par_slot, par_slot, zpeer[1])
    s5 = ship(5, par_slot, par_slot, zpeer[side - 1])
    turn(par_slot)
    landed(s1)
    s3 = ship(3, 2 * down + q, 2 * down + q, zpeer[1])
    turn(2 * down + q)
    landed(s4)
    turn(2 * up + q)
    landed(s5)
    s6 = ship(6, 2 * up + (1 - q), 2 * up + (1 - q), zpeer[side - 1])
    turn(2 * up + (1 - q))
    landed(s2)
    turn(2 * down + (1 - q))
    landed(s3)
    turn(2 * far + q)
    landed(s6)
    turn(2 * far + (1 - q))
    for pair in (s0, s1, s2, s3, s4, s5, s6):
        pair[0].wait_send()
        pair[1].wait_send()

    rowid = lax.broadcasted_iota(jnp.int32, (hs, LANE), 0)

    def z_copy(par, g, d):
        block = pl.ds(g * per_group, per_group)
        return remote(zbuf.at[par, zpos, block], zbuf.at[par, zpos, block],
                      zsend.at[par, g, d], zrecv.at[par, g, d], zpeer[d])

    def r_copy(d):
        return remote(gsend.at[(rpos + d) % side], rsbuf.at[rpos], rsend.at[d], rrecv.at[d], rpeer[d])

    def a_copy(d):
        return remote(wag.at[rpos], wag.at[rpos], asend.at[d], arecv.at[d], rpeer[d])

    def fin_ring(arr, d):
        return remote(fin.at[arr, q, zpos, rpos], fin.at[arr, q, zpos, rpos],
                      fsend.at[arr, d], frecv.at[arr, d], rpeer[d])

    def fin_cross(arr, d):
        return remote(fin.at[arr, q, zpos], fin.at[arr, q, zpos],
                      fsend.at[arr, side + d], frecv.at[arr, side + d], zpeer[d])

    def fin_pair(arr):
        return remote(fin.at[arr, q], fin.at[arr, q], fsend.at[arr, 0], frecv.at[arr, 0], partner)

    def gradient(k, _):
        par = k % 2
        w2z[...] = jnp.where(rowid >= cut, w2b[...], 0.0)

        def forward(g, _):
            for bb in range(per_group):
                b = g * per_group + bb
                off = pl.multiple_of(b * rows, rows)
                for n in range(rows // 256):
                    pre = jnp.dot(wb[...], xt[:, pl.ds(off + n * 256, 256)], preferred_element_type=f32)
                    act = jnp.tanh(pre)
                    abuf[b, :, n * 256:(n + 1) * 256] = act
                    for h in range(2):
                        part = jnp.sum(act[:, h * LANE:(h + 1) * LANE] * w2z[...], axis=0, keepdims=True)
                        zbuf[par, zpos, b, 2 * n + h:2 * n + h + 1, :] = part
            for d in range(1, side):
                z_copy(par, g, d).start()
            return 0

        lax.fori_loop(0, groups, forward, 0)
        gacc[...] = jnp.zeros_like(gacc)
        g2acc[...] = jnp.zeros_like(g2acc)

        def backward(g, _):
            for d in range(1, side):
                z_copy(par, g, d).wait_recv()
            for bb in range(per_group):
                b = g * per_group + bb
                off = pl.multiple_of(b * rows, rows)
                logit = zbuf[par, 0, b]
                for s in range(1, side):
                    logit = logit + zbuf[par, s, b]
                ztot[b] = logit
                res = ybuf[b].astype(f32) - jax.nn.sigmoid(logit)
                for n in range(nlt):
                    act = abuf[b, :, n * LANE:(n + 1) * LANE]
                    rr = jnp.broadcast_to(res[n:n + 1, :], (hs, LANE))
                    g2acc[...] += rr * act
                    bbuf[bb, :, n * LANE:(n + 1) * LANE] = ((rr * w2b[...]) * (1.0 - act * act)).astype(bf16)
                gacc[...] += jnp.dot(bbuf[bb], x[pl.ds(off, rows), :], preferred_element_type=f32)
            return 0

        lax.fori_loop(0, groups, backward, 0)
        pack(gacc, gsend, LANE)
        g2 = jnp.zeros((8, LANE), f32)
        for i in range(hs // 8):
            col = jnp.sum(g2acc[i * 8:(i + 1) * 8, :], axis=1, keepdims=True)
            g2 = jnp.where(lane8 == i, jnp.broadcast_to(col, (8, LANE)), g2)
        for o in range(side):
            gsend[o, urows:urows + 8, :] = g2
        for d in range(1, side):
            r_copy(d).start()
        rsbuf[rpos] = gsend[rpos]
        for g in range(groups):
            for d in range(1, side):
                z_copy(par, g, d).wait_send()
        for d in range(1, side):
            r_copy(d).wait_recv()
        total = rsbuf[0]
        for s in range(1, side):
            total = total + rsbuf[s]
        coef = jnp.where((k == 0) | (k == LEAPS), 0.5 * step, step).astype(f32)
        mom[...] = mom[...] + coef * (total[0:urows] - pos[...] / PRIOR_VAR)
        for i in range(hs // 8):
            blk = slice(i * 8, (i + 1) * 8)
            gcol = jnp.broadcast_to(total[urows:urows + 8, i:i + 1], (8, LANE))
            m2b[blk, :] = m2b[blk, :] + coef * (gcol - w2b[blk, :] / PRIOR_VAR)
        for d in range(1, side):
            r_copy(d).wait_send()

        @pl.when(k < LEAPS)
        def _():
            pos[...] = pos[...] + step * mom[...]
            w2b[...] = w2b[...] + step * m2b[...]
            wag[rpos] = pos[...].astype(bf16)
            for d in range(1, side):
                a_copy(d).start()
            for d in range(1, side):
                a_copy(d).wait_recv()
            for i in range(nrow):
                for kk in range(nfull):
                    o, j = unit_at(i * nfull + kk)
                    wb[i * PACK:(i + 1) * PACK, kk * LANE:(kk + 1) * LANE] = wag[o, j:j + PACK, :]
            o, j = unit_at(nunit - 1)
            left = wag[o, j:j + PACK, :].astype(f32)
            for i in range(nrow):
                v = pltpu.roll(left, LANE - i * rem, 1) if i else left
                wb[i * PACK:(i + 1) * PACK, nfull * LANE:] = jnp.where(lane < rem, v, 0.0).astype(bf16)
            for d in range(1, side):
                a_copy(d).wait_send()

        return 0

    lax.fori_loop(0, LEAPS + 1, gradient, 0)

    i0 = cut // PACK
    sq = jnp.zeros((PACK, LANE), f32)
    for j in range(own):
        u = own * rpos + j
        p_ = pos[j * PACK:(j + 1) * PACK, :]
        v_ = mom[j * PACK:(j + 1) * PACK, :]
        group_id = jnp.where(u == nunit - 1, lane // rem, u // nfull + 0 * lane)
        sq = sq + jnp.where(group_id >= i0, p_ * p_ / (2.0 * PRIOR_VAR) + 0.5 * (v_ * v_), 0.0)
    e_part = jnp.sum(sq, axis=(0, 1), keepdims=True)
    first = jnp.where((rowid >= cut) & (lax.broadcasted_iota(jnp.int32, (hs, LANE), 1) == 0),
                      w2b[...] * w2b[...] / (2.0 * PRIOR_VAR) + 0.5 * (m2b[...] * m2b[...]), 0.0)
    e_w2 = jnp.sum(first, axis=(0, 1), keepdims=True)
    loss = jnp.zeros((8, LANE), f32)
    for b in range(nshard):
        zt = ztot[b]
        loss = loss + (jnp.maximum(zt, 0.0) + jnp.log1p(jnp.exp(-jnp.abs(zt))) - ybuf[b].astype(f32) * zt)
    e_loss = jnp.sum(loss, axis=(0, 1), keepdims=True)
    e_part = e_part + jnp.where(rpos == 0, e_w2, 0.0) + jnp.where(zpos == 0, e_loss, 0.0)

    def as_row(ref):
        diag = jnp.where(rowid == lax.broadcasted_iota(jnp.int32, (hs, LANE), 1), ref[...], 0.0)
        return jnp.broadcast_to(jnp.sum(diag, axis=0, keepdims=True), (8, LANE))

    misc = jnp.where(sub8 == 0, as_row(w2b), jnp.where(sub8 == 1, as_row(m2b), jnp.broadcast_to(e_part, (8, LANE))))

    fin[0, q, zpos, rpos, 0:urows, :] = pos[...]
    fin[1, q, zpos, rpos, 0:urows, :] = mom[...]
    for arr in range(2):
        fin[arr, q, zpos, rpos, urows:urows + 8, :] = misc
    for make in (fin_ring, fin_cross):
        for arr in range(2):
            for d in range(1, side):
                make(arr, d).start()
        for arr in range(2):
            for d in range(1, side):
                make(arr, d).wait()
    for arr in range(2):
        fin_pair(arr).start()
    for arr in range(2):
        fin_pair(arr).wait()
    outs = []
    for arr, ref in ((0, fin_w), (1, fin_m)):
        for ch in range(2):
            for z in range(side):
                r0 = min(z * hs, hidden - hs)
                for i in range(nrow):
                    for k in range(nfull):
                        o, j = unit_at(i * nfull + k)
                        obuf[arr, ch, r0 + i * PACK:r0 + (i + 1) * PACK, k * LANE:(k + 1) * LANE] = fin[arr, ch, z, o, j:j + PACK, :]
                o, j = unit_at(nunit - 1)
                left = fin[arr, ch, z, o, j:j + PACK, :]
                for i in range(nrow):
                    v = pltpu.roll(left, LANE - i * rem, 1) if i else left
                    obuf[arr, ch, r0 + i * PACK:r0 + (i + 1) * PACK, nfull * LANE:feat] = v[:, 0:rem]
        cp = pltpu.make_async_copy(obuf.at[arr], ref, osem.at[arr])
        cp.start()
        outs.append(cp)
    for ch in range(2):
        for z in range(side):
            for r in range(side):
                misc_ref[ch, z, r] = fin[1, ch, z, r, urows:urows + 8, :]
    for cp in outs:
        cp.wait()


def solution(mesh):
    row_spec = P('data', None)
    label_spec = P('data')
    in_spec = P(None, 'parts', None)
    out_spec = P('parts', None)
    chain_spec = P('parts')
    side = math.isqrt(mesh.shape['data'] // 2)

    def run_chains(feats, labels, w_in, w_out, mom_in, mom_out):
        num_rows, feat = feats.shape
        hidden = w_in.shape[2]
        step = 1.0 / math.sqrt(num_rows * (feat + hidden))

        def device_body(x_rows, y_rows, pos_in, pos_out, vel_in, vel_out):
            rows = x_rows.shape[0]
            chains = pos_out.shape[0]
            hs = -(-(hidden // PACK) // side) * PACK
            kpad = -(-feat // LANE) * LANE
            nshard = 2 * side
            nfull = feat // LANE
            nunit = (hs // PACK) * nfull + 1
            urows = -(-nunit // side) * PACK
            groups = 4
            f32, bf16 = jnp.float32, jnp.bfloat16
            dma = pltpu.SemaphoreType.DMA
            vm = pltpu.VMEM
            cfg = (side, hidden, feat, rows, hs, step)
            full = jax.ShapeDtypeStruct((chains, hidden, feat), f32)
            any_spec = pl.BlockSpec(memory_space=pl.ANY)
            vmem_spec = pl.BlockSpec(memory_space=pltpu.VMEM)
            end_w, end_m, misc = pl.pallas_call(
                functools.partial(_kernel, cfg),
                out_shape=(full, full, jax.ShapeDtypeStruct((chains, side, side, 8, LANE), f32)),
                in_specs=[any_spec, vmem_spec, any_spec, any_spec, vmem_spec, vmem_spec],
                out_specs=(any_spec, any_spec, vmem_spec),
                scratch_shapes=[
                    vm((kpad, nshard * rows), bf16),
                    vm((nshard * rows, kpad), bf16),
                    vm((nshard, 8, rows // 8), jnp.int32),
                    vm((2, hs, feat), f32),
                    vm((hs, kpad), bf16),
                    vm((nshard, hs, rows), f32),
                    vm((nshard // groups, hs, rows), bf16),
                    vm((hs, kpad), f32),
                    vm((hs, LANE), f32),
                    vm((side, urows + 8, LANE), f32),
                    vm((side, urows + 8, LANE), f32),
                    vm((urows, LANE), f32),
                    vm((urows, LANE), f32),
                    vm((hs, LANE), f32),
                    vm((hs, LANE), f32),
                    vm((hs, LANE), f32),
                    vm((side, urows, LANE), bf16),
                    vm((2, side, nshard, 8, LANE), f32),
                    vm((nshard, 8, LANE), f32),
                    vm((2, chains, side, side, urows + 8, LANE), f32),
                    vm((2, chains, hidden, feat), f32),
                    dma((3,)), dma((7,)), dma((7,)), dma((7,)), dma((7,)),
                    dma((2, groups, side)), dma((2, groups, side)),
                    dma((side,)), dma((side,)), dma((side,)), dma((side,)),
                    dma((2, 2 * side)), dma((2, 2 * side)), dma((2,)),
                ],
                compiler_params=pltpu.CompilerParams(collective_id=0, has_side_effects=True, vmem_limit_bytes=67043328),
            )(x_rows.T, y_rows.reshape(8, rows // 8), pos_in.transpose(1, 2, 0), vel_in.transpose(1, 2, 0), pos_out, vel_out)
            keep = [misc[:, z, 0, 0:2, z * hs - min(z * hs, hidden - hs):hs] for z in range(side)]
            flat = jnp.concatenate(keep, axis=2)
            energy = jnp.sum(misc[:, :, :, 2, 0], axis=(1, 2))
            return end_w.transpose(2, 0, 1), flat[:, 0], end_m.transpose(2, 0, 1), flat[:, 1], energy

        mapped = jax.shard_map(device_body, mesh=mesh, in_specs=(row_spec, label_spec, in_spec, out_spec, in_spec, out_spec), out_specs=(in_spec, out_spec, in_spec, out_spec, chain_spec), check_vma=False)
        return mapped(feats, labels, w_in, w_out, mom_in, mom_out)

    return run_chains
```

```python
import functools
import math

import jax
import jax.numpy as jnp
from jax import lax
from jax.experimental import pallas as pl
from jax.experimental.pallas import tpu as pltpu
from jax.sharding import PartitionSpec as P

LEAPS = 16
PRIOR_VAR = 1.0
LANE = 128
PACK = 16
MESH_ID = pl.DeviceIdType.MESH


def _kernel(cfg, xt_hbm, lab_ref, w_hbm, m_hbm, wo_ref, mo_ref, fin,
            xt, x, ybuf, wload, wb, abuf, bbuf, gacc, g2acc, gsend, rsbuf, pos, mom, w2b, m2b, w2z, wag, zbuf, ztot,
            lsem, isend, irecv, ysend, yrecv, zsend, zrecv, rsend, rrecv, asend, arecv, fsend, frecv,
            csend, crecv, psend, precv):
    side, hidden, feat, rows, hs, step = cfg
    half = side // 2
    nshard = 2 * side
    nfull = feat // LANE
    rem = feat - nfull * LANE
    nrow = hs // PACK
    nunit = nrow * nfull + 1
    own = -(-nunit // side)
    urows = own * PACK
    kpad = xt.shape[0]
    nlt = rows // LANE
    groups = zsend.shape[1]
    per_group = nshard // groups
    f32, bf16 = jnp.float32, jnp.bfloat16

    me = lax.axis_index('data')
    core = me % 2
    xx = (me // 2) % side
    yy = me // (2 * side)

    def fold(y, x_):
        return (x_ // half + y // half) % 2

    q = (core + fold(yy, xx)) % 2
    zpos = xx * (1 - q) + yy * q
    rpos = yy * (1 - q) + xx * q

    def device(z, r, role):
        x2 = z * (1 - role) + r * role
        y2 = r * (1 - role) + z * role
        return {'data': (y2 * side + x2) * 2 + (role + fold(y2, x2)) % 2}

    zpeer = [device((zpos + d) % side, rpos, q) for d in range(side)]
    rpeer = [device(zpos, (rpos + d) % side, q) for d in range(side)]
    partner = device(rpos, zpos, 1 - q)

    def remote(src, dst, ssem, rsem, dev):
        return pltpu.make_async_remote_copy(src_ref=src, dst_ref=dst, send_sem=ssem, recv_sem=rsem,
                                            device_id=dev, device_id_type=MESH_ID)

    start = jnp.minimum(zpos * hs, hidden - hs)
    start = pl.multiple_of(start, 8)
    cut = zpos * hs - start

    own_slot = 2 * zpos + q
    par_slot = 2 * zpos + (1 - q)

    parts = isend.shape[1]
    piece = rows // parts
    order = [d for d in range(1, side) if d == half] + [d for d in range(1, side) if d != half]

    def xcols(slot, h):
        return xt.at[pl.ds(0, feat), pl.ds(pl.multiple_of(slot * rows + h * piece, piece), piece)]

    load_x = pltpu.make_async_copy(xt_hbm, xt.at[pl.ds(0, feat), pl.ds(pl.multiple_of(own_slot * rows, rows), rows)], lsem.at[0])
    load_w = pltpu.make_async_copy(w_hbm.at[q, pl.ds(start, hs), :], wload.at[0], lsem.at[1])
    load_m = pltpu.make_async_copy(m_hbm.at[q, pl.ds(start, hs), :], wload.at[1], lsem.at[2])
    load_x.start()
    load_w.start()
    load_m.start()

    barrier = pltpu.get_barrier_semaphore()
    for dev in zpeer[1:] + rpeer[1:] + [partner]:
        pl.semaphore_signal(barrier, inc=1, device_id=dev, device_id_type=MESH_ID)
    pl.semaphore_wait(barrier, 2 * side - 1)

    class Ship:
        def __init__(self, i, slot, dslot, dev):
            self.x = [remote(xcols(slot, h), xcols(dslot, h), isend.at[i, h], irecv.at[i, h], dev) for h in range(parts)]
            self.y = remote(ybuf.at[slot], ybuf.at[dslot], ysend.at[i], yrecv.at[i], dev)

        def start(self, h):
            self.x[h].start()
            if h == parts - 1:
                self.y.start()

        def landed(self, h):
            self.x[h].wait_recv()
            if h == parts - 1:
                self.y.wait_recv()

        def sent(self):
            for c in self.x:
                c.wait_send()
            self.y.wait_send()

    def turn(slot):
        def body(t, _):
            off = pl.multiple_of(slot * rows + t * LANE, LANE)
            x[pl.ds(off, LANE), :] = xt[:, pl.ds(off, LANE)].T
            return 0
        lax.fori_loop(0, rows // LANE, body, 0)

    ybuf[own_slot] = lab_ref[...]
    up, down, far = (zpos + 1) % side, (zpos + side - 1) % side, (zpos + 2) % side
    forth, back = zpeer[1], zpeer[side - 1]
    s0 = Ship(0, own_slot, 2 * rpos + q, partner)
    s1 = Ship(1, own_slot, own_slot, forth)
    s2 = Ship(2, par_slot, par_slot, forth)
    s3 = Ship(3, 2 * down + q, 2 * down + q, forth)
    s4 = Ship(4, own_slot, own_slot, back)
    s5 = Ship(5, par_slot, par_slot, back)
    s6 = Ship(6, 2 * up + (1 - q), 2 * up + (1 - q), back)
    load_x.wait()
    for h in range(parts):
        for ship in (s0, s1, s4):
            ship.start(h)
    xt[feat:kpad, :] = jnp.zeros((kpad - feat, nshard * rows), bf16)
    turn(own_slot)

    lane = lax.broadcasted_iota(jnp.int32, (PACK, LANE), 1)
    lane8 = lax.broadcasted_iota(jnp.int32, (8, LANE), 1)
    sub8 = lax.broadcasted_iota(jnp.int32, (8, LANE), 0)

    def unit_at(u):
        return u // own, (u % own) * PACK

    def pack(src, dst, width):
        for i in range(nrow):
            for k in range(nfull):
                o, j = unit_at(i * nfull + k)
                dst[o, j:j + PACK, :] = src[i * PACK:(i + 1) * PACK, k * LANE:(k + 1) * LANE]
        o, j = unit_at(nunit - 1)
        acc = jnp.zeros((PACK, LANE), f32)
        for i in range(nrow):
            v = src[i * PACK:(i + 1) * PACK, nfull * LANE:nfull * LANE + width]
            if width < LANE:
                v = jnp.concatenate([v, jnp.zeros((PACK, LANE - width), f32)], axis=1)
            acc = acc + (pltpu.roll(v, i * rem, 1) if i else v)
        dst[o, j:j + PACK, :] = acc

    for o in range(side):
        for u in range(nunit, side * own):
            if u // own == o:
                gsend[o, (u % own) * PACK:(u % own + 1) * PACK, :] = jnp.zeros((PACK, LANE), f32)
    load_w.wait()
    load_m.wait()
    pack(wload.at[1], gsend, rem)
    mom[...] = gsend[rpos, 0:urows, :]
    pack(wload.at[0], gsend, rem)
    pos[...] = gsend[rpos, 0:urows, :]
    wb[:, nfull * LANE:] = jnp.zeros((hs, kpad - nfull * LANE), bf16)
    wb[:, 0:feat] = wload[0].astype(bf16)

    def column(ref, dst):
        width = -(-hidden // LANE) * LANE
        v = jnp.concatenate([ref[pl.ds(q, 1), :], jnp.zeros((1, width - hidden), f32)], axis=1)
        lanes = lax.broadcasted_iota(jnp.int32, (8, width), 1)
        subs = lax.broadcasted_iota(jnp.int32, (8, width), 0)
        v = jnp.broadcast_to(v, (8, width))
        for i in range(hs // 8):
            hit = jnp.where(lanes == start + i * 8 + subs, v, 0.0)
            dst[i * 8:(i + 1) * 8, :] = jnp.broadcast_to(jnp.sum(hit, axis=1, keepdims=True), (8, LANE))

    column(wo_ref, w2b)
    column(mo_ref, m2b)

    rowid = lax.broadcasted_iota(jnp.int32, (hs, LANE), 0)

    def hidden_block(par, b, off):
        for n in range(rows // 256):
            pre = jnp.dot(wb[...], xt[:, pl.ds(off + n * 256, 256)], preferred_element_type=f32)
            act = jnp.tanh(pre)
            abuf[b, :, n * 256:(n + 1) * 256] = act
            for h in range(2):
                part = jnp.sum(act[:, h * LANE:(h + 1) * LANE] * w2z[...], axis=0, keepdims=True)
                zbuf[par, zpos, b, 2 * n + h:2 * n + h + 1, :] = part

    def first_pass(slot):
        hidden_block(0, slot, pl.multiple_of(slot * rows, rows))

    w2z[...] = jnp.where(rowid >= cut, w2b[...], 0.0)
    for h in range(parts):
        s0.landed(h)
        s2.start(h)
        s5.start(h)
    turn(par_slot)
    first_pass(own_slot)
    first_pass(par_slot)
    for h in range(parts):
        s1.landed(h)
        s3.start(h)
    turn(2 * down + q)
    first_pass(2 * down + q)
    for h in range(parts):
        s4.landed(h)
    turn(2 * up + q)
    first_pass(2 * up + q)
    for h in range(parts):
        s5.landed(h)
        s6.start(h)
    turn(2 * up + (1 - q))
    first_pass(2 * up + (1 - q))
    for h in range(parts):
        s2.landed(h)
    turn(2 * down + (1 - q))
    first_pass(2 * down + (1 - q))
    for h in range(parts):
        s3.landed(h)
    turn(2 * far + q)
    first_pass(2 * far + q)
    for h in range(parts):
        s6.landed(h)
    turn(2 * far + (1 - q))
    first_pass(2 * far + (1 - q))

    def z_copy(par, g, d):
        block = pl.ds(g * per_group, per_group)
        return remote(zbuf.at[par, zpos, block], zbuf.at[par, zpos, block],
                      zsend.at[par, g, d], zrecv.at[par, g, d], zpeer[d])

    def r_copy(d):
        return remote(gsend.at[(rpos + d) % side], rsbuf.at[rpos], rsend.at[d], rrecv.at[d], rpeer[d])

    def a_copy(d):
        return remote(wag.at[rpos], wag.at[rpos], asend.at[d], arecv.at[d], rpeer[d])

    def fin_ring(arr, d):
        return remote(fin.at[arr, q, zpos, rpos], fin.at[arr, q, zpos, rpos], fsend.at[arr, d], frecv.at[arr, d], rpeer[d])

    def fin_cross(arr, e, d):
        block = fin.at[arr, q, zpos, (rpos + e) % side]
        return remote(block, block, csend.at[arr, e, d], crecv.at[arr, e, d], zpeer[d])

    def fin_pair(arr, w):
        block = fin.at[arr, q, (zpos + w) % side]
        return remote(block, block, psend.at[arr, w], precv.at[arr, w], partner)

    def spread(arr):
        for d in order:
            fin_ring(arr, d).start()
        for d in order:
            fin_cross(arr, 0, d).start()

    def relay(arr):
        for d in reversed(order):
            fin_ring(arr, d).wait_recv()
            for dd in order:
                fin_cross(arr, side - d, dd).start()

    def over(arr):
        fin_pair(arr, 0).start()
        for w in reversed(order):
            for e in range(side):
                fin_cross(arr, e, side - w).wait_recv()
            fin_pair(arr, w).start()

    for g in range(groups):
        for d in order:
            z_copy(0, g, d).start()
    for ship in (s0, s1, s2, s3, s4, s5, s6):
        ship.sent()

    def gradient(k, _):
        par = k % 2
        gacc[...] = jnp.zeros_like(gacc)
        g2acc[...] = jnp.zeros_like(g2acc)

        def backward(g):
            for d in range(1, side):
                z_copy(par, g, d).wait_recv()
            for bb in range(per_group):
                b = g * per_group + bb
                off = b * rows
                logit = zbuf[par, 0, b]
                for s in range(1, side):
                    logit = logit + zbuf[par, s, b]
                ztot[b] = logit
                res = ybuf[b].astype(f32) - jax.nn.sigmoid(logit)
                for n in range(nlt):
                    act = abuf[b, :, n * LANE:(n + 1) * LANE]
                    rr = jnp.broadcast_to(res[n:n + 1, :], (hs, LANE))
                    g2acc[...] += rr * act
                    bbuf[bb, :, n * LANE:(n + 1) * LANE] = ((rr * w2b[...]) * (1.0 - act * act)).astype(bf16)
                for lo in range(0, kpad, 256):
                    hi = min(lo + 256, kpad)
                    gacc[:, lo:hi] += jnp.dot(bbuf[bb], x[off:off + rows, lo:hi], preferred_element_type=f32)

        for g in range(groups):
            backward(g)
        pack(gacc, gsend, LANE)
        g2 = jnp.zeros((8, LANE), f32)
        for i in range(hs // 8):
            col = jnp.sum(g2acc[i * 8:(i + 1) * 8, :], axis=1, keepdims=True)
            g2 = jnp.where(lane8 == i, jnp.broadcast_to(col, (8, LANE)), g2)
        for o in range(side):
            gsend[o, urows:urows + 8, :] = g2
        for d in order:
            r_copy(d).start()
        rsbuf[rpos] = gsend[rpos]
        for g in range(groups):
            for d in range(1, side):
                z_copy(par, g, d).wait_send()
        for d in range(1, side):
            r_copy(d).wait_recv()
        total = rsbuf[0]
        for s in range(1, side):
            total = total + rsbuf[s]
        coef = jnp.where((k == 0) | (k == LEAPS), 0.5 * step, step).astype(f32)
        mom[...] = mom[...] + coef * (total[0:urows] - pos[...] / PRIOR_VAR)
        for i in range(hs // 8):
            blk = slice(i * 8, (i + 1) * 8)
            gcol = jnp.broadcast_to(total[urows:urows + 8, i:i + 1], (8, LANE))
            m2b[blk, :] = m2b[blk, :] + coef * (gcol - w2b[blk, :] / PRIOR_VAR)
        for d in range(1, side):
            r_copy(d).wait_send()

        @pl.when(k < LEAPS)
        def _():
            pos[...] = pos[...] + step * mom[...]
            w2b[...] = w2b[...] + step * m2b[...]
            wag[rpos] = pos[...].astype(bf16)
            for d in order:
                a_copy(d).start()

            @pl.when(k == LEAPS - 1)
            def _():
                fin[0, q, zpos, rpos, 0:urows, :] = pos[...]
                fin[0, q, zpos, rpos, urows:urows + 8, :] = jnp.zeros((8, LANE), f32)
                spread(0)

            for d in range(1, side):
                a_copy(d).wait_recv()
            for i in range(nrow):
                for kk in range(nfull):
                    o, j = unit_at(i * nfull + kk)
                    wb[i * PACK:(i + 1) * PACK, kk * LANE:(kk + 1) * LANE] = wag[o, j:j + PACK, :]
            o, j = unit_at(nunit - 1)
            left = wag[o, j:j + PACK, :].astype(f32)
            for i in range(nrow):
                v = pltpu.roll(left, LANE - i * rem, 1) if i else left
                wb[i * PACK:(i + 1) * PACK, nfull * LANE:] = jnp.where(lane < rem, v, 0.0).astype(bf16)
            w2z[...] = jnp.where(rowid >= cut, w2b[...], 0.0)
            for g in range(groups):
                for b in range(g * per_group, (g + 1) * per_group):
                    hidden_block(1 - par, b, b * rows)
                for d in order:
                    z_copy(1 - par, g, d).start()
            for d in range(1, side):
                a_copy(d).wait_send()

            @pl.when(k == LEAPS - 1)
            def _():
                relay(0)

        return 0

    lax.fori_loop(0, LEAPS + 1, gradient, 0)

    i0 = cut // PACK
    sq = jnp.zeros((PACK, LANE), f32)
    for j in range(own):
        u = own * rpos + j
        p_ = pos[j * PACK:(j + 1) * PACK, :]
        v_ = mom[j * PACK:(j + 1) * PACK, :]
        group_id = jnp.where(u == nunit - 1, lane // rem, u // nfull + 0 * lane)
        sq = sq + jnp.where(group_id >= i0, p_ * p_ / (2.0 * PRIOR_VAR) + 0.5 * (v_ * v_), 0.0)
    e_part = jnp.sum(sq, axis=(0, 1), keepdims=True)
    first = jnp.where((rowid >= cut) & (lax.broadcasted_iota(jnp.int32, (hs, LANE), 1) == 0),
                      w2b[...] * w2b[...] / (2.0 * PRIOR_VAR) + 0.5 * (m2b[...] * m2b[...]), 0.0)
    e_w2 = jnp.sum(first, axis=(0, 1), keepdims=True)
    loss = jnp.zeros((8, LANE), f32)
    for b in range(nshard):
        zt = ztot[b]
        loss = loss + (jnp.maximum(zt, 0.0) + jnp.log1p(jnp.exp(-jnp.abs(zt))) - ybuf[b].astype(f32) * zt)
    e_loss = jnp.sum(loss, axis=(0, 1), keepdims=True)
    e_part = e_part + jnp.where(rpos == 0, e_w2, 0.0) + jnp.where(zpos == 0, e_loss, 0.0)

    def as_row(ref):
        diag = jnp.where(rowid == lax.broadcasted_iota(jnp.int32, (hs, LANE), 1), ref[...], 0.0)
        return jnp.broadcast_to(jnp.sum(diag, axis=0, keepdims=True), (8, LANE))

    misc = jnp.where(sub8 == 0, as_row(w2b), jnp.where(sub8 == 1, as_row(m2b), jnp.broadcast_to(e_part, (8, LANE))))

    fin[1, q, zpos, rpos, 0:urows, :] = mom[...]
    fin[1, q, zpos, rpos, urows:urows + 8, :] = misc
    spread(1)
    over(0)
    relay(1)
    over(1)
    for arr in range(2):
        for w in range(side):
            fin_pair(arr, w).wait()
        for d in order:
            fin_ring(arr, d).wait_send()
            for e in range(side):
                fin_cross(arr, e, d).wait_send()


def _unpack(cfg, packed, end_w, end_m, w_row, m_row, energy, fin, obuf, lsem, sem):
    side, hidden, feat, rows, hs, step = cfg
    chains = fin.shape[1]
    nfull = feat // LANE
    rem = feat - nfull * LANE
    nrow = hs // PACK
    nunit = nrow * nfull + 1
    own = -(-nunit // side)
    urows = own * PACK
    f32 = jnp.float32
    copies = []
    loads = {(arr, ch): pltpu.make_async_copy(packed.at[arr, ch], fin.at[arr, ch], lsem.at[arr, ch]) for arr in range(2) for ch in range(chains)}
    for ld in loads.values():
        ld.start()
    for arr, ref in ((0, end_w), (1, end_m)):
        for ch in range(chains):
            loads[arr, ch].wait()
            for z in range(side):
                r0 = min(z * hs, hidden - hs)
                for i in range(nrow):
                    r1 = r0 + i * PACK
                    for k in range(nfull):
                        u = i * nfull + k
                        obuf[arr, ch, r1:r1 + PACK, k * LANE:(k + 1) * LANE] = fin[arr, ch, z, u // own, (u % own) * PACK:(u % own + 1) * PACK, :]
                u = nunit - 1
                left = fin[arr, ch, z, u // own, (u % own) * PACK:(u % own + 1) * PACK, :]
                for i in range(nrow):
                    v = pltpu.roll(left, LANE - i * rem, 1) if i else left
                    obuf[arr, ch, r0 + i * PACK:r0 + (i + 1) * PACK, nfull * LANE:feat] = v[:, 0:rem]
            cp = pltpu.make_async_copy(obuf.at[arr, ch], ref.at[ch], sem.at[arr, ch])
            cp.start()
            copies.append(cp)
    width = -(-hidden // LANE) * LANE
    lane = lax.broadcasted_iota(jnp.int32, (8, width), 1)
    for ch in range(chains):
        acc = jnp.zeros((8, width), f32)
        tot = jnp.zeros((8, LANE), f32)
        for z in range(side):
            tile = fin[1, ch, z, 0, urows:urows + 8, :]
            wide = jnp.concatenate([tile, jnp.zeros((8, width - LANE), f32)], axis=1)
            r0 = min(z * hs, hidden - hs)
            wide = pltpu.roll(wide, r0, 1) if r0 else wide
            acc = jnp.where((lane >= z * hs) & (lane < (z + 1) * hs), wide, acc)
            for r in range(side):
                tot = tot + fin[1, ch, z, r, urows:urows + 8, :]
        w_row[ch:ch + 1, :] = acc[0:1, 0:hidden]
        m_row[ch:ch + 1, :] = acc[1:2, 0:hidden]
        energy[ch] = jnp.sum(tot[2:3, 0:1])
    for cp in copies:
        cp.wait()


def solution(mesh):
    row_spec = P('data', None)
    label_spec = P('data')
    in_spec = P(None, 'parts', None)
    out_spec = P('parts', None)
    chain_spec = P('parts')
    side = math.isqrt(mesh.shape['data'] // 2)

    def run_chains(feats, labels, w_in, w_out, mom_in, mom_out):
        num_rows, feat = feats.shape
        hidden = w_in.shape[2]
        step = 1.0 / math.sqrt(num_rows * (feat + hidden))

        def device_body(x_rows, y_rows, pos_in, pos_out, vel_in, vel_out):
            rows = x_rows.shape[0]
            chains = pos_out.shape[0]
            hs = -(-(hidden // PACK) // side) * PACK
            kpad = -(-feat // LANE) * LANE
            nshard = 2 * side
            nfull = feat // LANE
            nunit = (hs // PACK) * nfull + 1
            urows = -(-nunit // side) * PACK
            groups = 4
            f32, bf16 = jnp.float32, jnp.bfloat16
            dma = pltpu.SemaphoreType.DMA
            vm = pltpu.VMEM
            cfg = (side, hidden, feat, rows, hs, step)
            full = jax.ShapeDtypeStruct((chains, hidden, feat), f32)
            any_spec = pl.BlockSpec(memory_space=pl.ANY)
            vmem_spec = pl.BlockSpec(memory_space=pltpu.VMEM)
            piece_shape = (2, chains, side, side, urows + 8, LANE)
            fin = pl.pallas_call(
                functools.partial(_kernel, cfg),
                out_shape=jax.ShapeDtypeStruct(piece_shape, f32),
                in_specs=[any_spec, vmem_spec, any_spec, any_spec, vmem_spec, vmem_spec],
                out_specs=vmem_spec,
                scratch_shapes=[
                    vm((kpad, nshard * rows), bf16),
                    vm((nshard * rows, kpad), bf16),
                    vm((nshard, 8, rows // 8), jnp.int32),
                    vm((2, hs, feat), f32),
                    vm((hs, kpad), bf16),
                    vm((nshard, hs, rows), f32),
                    vm((nshard // groups, hs, rows), bf16),
                    vm((hs, kpad), f32),
                    vm((hs, LANE), f32),
                    vm((side, urows + 8, LANE), f32),
                    vm((side, urows + 8, LANE), f32),
                    vm((urows, LANE), f32),
                    vm((urows, LANE), f32),
                    vm((hs, LANE), f32),
                    vm((hs, LANE), f32),
                    vm((hs, LANE), f32),
                    vm((side, urows, LANE), bf16),
                    vm((2, side, nshard, 8, LANE), f32),
                    vm((nshard, 8, LANE), f32),
                    dma((3,)), dma((7, 2)), dma((7, 2)), dma((7,)), dma((7,)),
                    dma((2, groups, side)), dma((2, groups, side)),
                    dma((side,)), dma((side,)), dma((side,)), dma((side,)),
                    dma((2, side)), dma((2, side)), dma((2, side, side)), dma((2, side, side)),
                    dma((2, side)), dma((2, side)),
                ],
                compiler_params=pltpu.CompilerParams(collective_id=0, has_side_effects=True, vmem_limit_bytes=67043328),
            )(x_rows.T, y_rows.reshape(8, rows // 8), pos_in.transpose(1, 2, 0), vel_in.transpose(1, 2, 0), pos_out, vel_out)
            end_w, end_m, w_row, m_row, energy = pl.pallas_call(
                functools.partial(_unpack, cfg),
                out_shape=(full, full, jax.ShapeDtypeStruct((chains, hidden), f32), jax.ShapeDtypeStruct((chains, hidden), f32),
                           jax.ShapeDtypeStruct((chains,), f32)),
                in_specs=[any_spec],
                out_specs=(any_spec, any_spec, vmem_spec, vmem_spec, pl.BlockSpec(memory_space=pltpu.SMEM)),
                scratch_shapes=[vm(piece_shape, f32), vm((2, chains, hidden, feat), f32), dma((2, chains)), dma((2, chains))],
                compiler_params=pltpu.CompilerParams(vmem_limit_bytes=67043328),
            )(fin)
            return end_w.transpose(2, 0, 1), w_row, end_m.transpose(2, 0, 1), m_row, energy

        mapped = jax.shard_map(device_body, mesh=mesh, in_specs=(row_spec, label_spec, in_spec, out_spec, in_spec, out_spec), out_specs=(in_spec, out_spec, in_spec, out_spec, chain_spec), check_vma=False)
        return mapped(feats, labels, w_in, w_out, mom_in, mom_out)

    return run_chains
```

```python
import functools
import math

import jax
import jax.numpy as jnp
from jax import lax
from jax.experimental import pallas as pl
from jax.experimental.pallas import tpu as pltpu
from jax.sharding import PartitionSpec as P

LEAPS = 16
PRIOR_VAR = 1.0
LANE = 128
MESH_ID = pl.DeviceIdType.MESH


class Tiles:
    def __init__(self, side, feat, hs):
        self.nrow = hs // 8
        self.nfull = feat // LANE
        self.rem = feat - self.nfull * LANE
        self.per = LANE // self.rem
        split = 2 * (self.nfull // 3)
        self.lanes = split * LANE
        left = [(None, j) for j in range(-(-self.nrow // self.per))]
        self.part = [[(i, k) for i in range(self.nrow) for k in range(split)],
                     [(i, k) for i in range(self.nrow) for k in range(split, self.nfull)] + left]
        self.count = [len(p) // side for p in self.part]
        assert all(len(p) % side == 0 for p in self.part)
        self.size = [8 * n for n in self.count]

    def value(self, src, tile):
        i, k = tile
        if i is not None:
            return src[8 * i:8 * i + 8, k * LANE:(k + 1) * LANE]
        acc = None
        for g in range(min(self.per, self.nrow - k * self.per)):
            i = k * self.per + g
            v = src[8 * i:8 * i + 8, self.nfull * LANE:src.shape[1]]
            if v.shape[1] < LANE:
                v = jnp.concatenate([v, jnp.zeros((8, LANE - v.shape[1]), v.dtype)], axis=1)
            v = pltpu.roll(v, g * self.rem, 1) if g else v
            acc = v if acc is None else acc + v
        return acc


def _kernel(cfg, xt_hbm, lab_hbm, w_hbm, m_hbm, wo_hbm, mo_hbm, fin,
            xt, x, ybuf, oload, estage, g2sum, wload, wb, abuf, bbuf, gacc, g2acc, gsend_a, gsend_b, rsum_a, rsum_b, pos, mom, w2b, m2b, w2z,
            wag_a, wag_b, zbuf, ztot,
            lsem, isend, irecv, ysend, yrecv, zsend, zrecv, rsend, rrecv, asend, arecv, fsend, frecv,
            csend, crecv, psend, precv):
    side, hidden, feat, rows, hs, step, sizes = cfg
    half = side // 2
    nshard = 2 * side
    tiles = Tiles(side, feat, hs)
    nfull, rem = tiles.nfull, tiles.rem
    size_a, size_b = tiles.size
    urows = size_a + size_b
    gsend, rsum, wag = (gsend_a, gsend_b), (rsum_a, rsum_b), (wag_a, wag_b)
    span = (slice(0, size_a), slice(size_a, urows))
    kpad = xt.shape[0]
    nlt = rows // LANE
    groups = len(sizes)
    blocks = [range(sum(sizes[:g]), sum(sizes[:g + 1])) for g in range(groups)]
    f32, bf16 = jnp.float32, jnp.bfloat16

    me = lax.axis_index('data')
    core = me % 2
    xx = (me // 2) % side
    yy = me // (2 * side)

    def fold(y, x_):
        return (x_ // half + y // half) % 2

    q = (core + fold(yy, xx)) % 2
    zpos = xx * (1 - q) + yy * q
    rpos = yy * (1 - q) + xx * q

    def device(z, r, role):
        x2 = z * (1 - role) + r * role
        y2 = r * (1 - role) + z * role
        return {'data': (y2 * side + x2) * 2 + (role + fold(y2, x2)) % 2}

    zpeer = [device((zpos + d) % side, rpos, q) for d in range(side)]
    rpeer = [device(zpos, (rpos + d) % side, q) for d in range(side)]
    partner = device(rpos, zpos, 1 - q)

    def remote(src, dst, ssem, rsem, dev):
        return pltpu.make_async_remote_copy(src_ref=src, dst_ref=dst, send_sem=ssem, recv_sem=rsem,
                                            device_id=dev, device_id_type=MESH_ID)

    start = jnp.minimum(zpos * hs, hidden - hs)
    start = pl.multiple_of(start, 8)
    cut = zpos * hs - start

    own_slot = 2 * zpos + q
    par_slot = 2 * zpos + (1 - q)

    parts = isend.shape[1]
    piece = rows // parts
    order = [d for d in range(1, side) if d == half] + [d for d in range(1, side) if d != half]

    def xcols(slot, h):
        return xt.at[pl.ds(0, feat), pl.ds(pl.multiple_of(slot * rows + h * piece, piece), piece)]

    load_x = [pltpu.make_async_copy(xt_hbm.at[:, pl.ds(h * piece, piece)], xcols(own_slot, h), lsem.at[2 + h]) for h in range(parts)]
    load_w = pltpu.make_async_copy(w_hbm.at[q, pl.ds(start, hs), :], wload.at[0], lsem.at[0])
    load_m = pltpu.make_async_copy(m_hbm.at[q, pl.ds(start, hs), :], wload.at[1], lsem.at[1])
    load_y = pltpu.make_async_copy(lab_hbm, ybuf.at[own_slot], ysend.at[7])
    load_o = [pltpu.make_async_copy(src, oload.at[i], yrecv.at[7 + i]) for i, src in enumerate((wo_hbm, mo_hbm))]
    for cp in load_x + [load_y, load_w, load_m] + load_o:
        cp.start()

    barrier = pltpu.get_barrier_semaphore()
    for dev in zpeer[1:] + rpeer[1:] + [partner]:
        pl.semaphore_signal(barrier, inc=1, device_id=dev, device_id_type=MESH_ID)
    pl.semaphore_wait(barrier, 2 * side - 1)

    class Ship:
        def __init__(self, i, slot, dslot, dev):
            self.x = [remote(xcols(slot, h), xcols(dslot, h), isend.at[i, h], irecv.at[i, h], dev) for h in range(parts)]
            self.y = remote(ybuf.at[slot], ybuf.at[dslot], ysend.at[i], yrecv.at[i], dev)

        def start(self, h):
            self.x[h].start()
            if h == parts - 1:
                self.y.start()

        def landed(self, h):
            self.x[h].wait_recv()
            if h == parts - 1:
                self.y.wait_recv()

        def sent(self):
            for c in self.x:
                c.wait_send()
            self.y.wait_send()

    def turn(slot, h):
        def body(t, _):
            off = pl.multiple_of(slot * rows + h * piece + t * LANE, LANE)
            x[pl.ds(off, LANE), :] = xt[:, pl.ds(off, LANE)].T
            return 0
        lax.fori_loop(0, piece // LANE, body, 0)

    up, down, far = (zpos + 1) % side, (zpos + side - 1) % side, (zpos + 2) % side
    forth, back = zpeer[1], zpeer[side - 1]
    s0 = Ship(0, own_slot, 2 * rpos + q, partner)
    s1 = Ship(1, own_slot, own_slot, forth)
    s2 = Ship(2, par_slot, par_slot, forth)
    s3 = Ship(3, 2 * down + q, 2 * down + q, forth)
    s4 = Ship(4, own_slot, own_slot, back)
    s5 = Ship(5, par_slot, par_slot, back)
    s6 = Ship(6, 2 * up + (1 - q), 2 * up + (1 - q), back)
    load_y.wait()
    for h in range(parts):
        load_x[h].wait()
        for ship in (s0, s1, s4):
            ship.start(h)
    xt[feat:kpad, :] = jnp.zeros((kpad - feat, nshard * rows), bf16)
    for h in range(parts):
        turn(own_slot, h)

    lane8 = lax.broadcasted_iota(jnp.int32, (8, LANE), 1)
    sub8 = lax.broadcasted_iota(jnp.int32, (8, LANE), 0)

    def pack(p, src):
        n = tiles.count[p]
        for t, tile in enumerate(tiles.part[p]):
            gsend[p][t // n, 8 * (t % n):8 * (t % n) + 8, :] = tiles.value(src, tile)

    def adopt(p, src):
        n = tiles.count[p]
        held = [src[o].astype(f32) for o in range(side)]
        got = {tile: held[t // n][8 * (t % n):8 * (t % n) + 8] for t, tile in enumerate(tiles.part[p])}
        for k in sorted({k for i, k in tiles.part[p] if i is not None}):
            for i in range(0, tiles.nrow, 2):
                v = got[i, k] if i + 1 == tiles.nrow else jnp.concatenate([got[i, k], got[i + 1, k]], axis=0)
                wb[8 * i:8 * i + v.shape[0], k * LANE:(k + 1) * LANE] = v.astype(bf16)
        if (None, 0) in got:
            def left(i):
                g = i % tiles.per
                v = got[None, i // tiles.per]
                v = pltpu.roll(v, LANE - g * rem, 1) if g else v
                return jnp.where(lane8 < rem, v, 0.0)
            for i in range(0, tiles.nrow, 2):
                v = left(i) if i + 1 == tiles.nrow else jnp.concatenate([left(i), left(i + 1)], axis=0)
                wb[8 * i:8 * i + v.shape[0], nfull * LANE:] = v.astype(bf16)

    load_w.wait()
    load_m.wait()
    for src, dst in ((1, mom), (0, pos)):
        for p in range(2):
            pack(p, wload.at[src])
            dst[span[p], :] = gsend[p][rpos, 0:tiles.size[p], :]
    wb[:, nfull * LANE:] = jnp.zeros((hs, kpad - nfull * LANE), bf16)
    wb[:, 0:feat] = wload[0].astype(bf16)

    def column(ref, dst):
        width = -(-hidden // LANE) * LANE
        v = jnp.concatenate([oload[ref, pl.ds(q, 1), :], jnp.zeros((1, width - hidden), f32)], axis=1)
        lanes = lax.broadcasted_iota(jnp.int32, (8, width), 1)
        subs = lax.broadcasted_iota(jnp.int32, (8, width), 0)
        v = jnp.broadcast_to(v, (8, width))
        for i in range(hs // 8):
            hit = jnp.where(lanes == start + i * 8 + subs, v, 0.0)
            dst[i * 8:(i + 1) * 8, :] = jnp.broadcast_to(jnp.sum(hit, axis=1, keepdims=True), (8, LANE))

    for cp in load_o:
        cp.wait()
    column(0, w2b)
    column(1, m2b)

    rowid = lax.broadcasted_iota(jnp.int32, (hs, LANE), 0)

    def hidden_block(par, b, off, first, last, done=0):
        for n in range(first, last):
            pre = jnp.dot(wb[:, done:], xt[done:, pl.ds(off + n * 256, 256)], preferred_element_type=f32)
            if done:
                pre = pre + abuf[b, :, n * 256:(n + 1) * 256]
            act = jnp.tanh(pre)
            abuf[b, :, n * 256:(n + 1) * 256] = act
            for h in range(2):
                part = jnp.sum(act[:, h * LANE:(h + 1) * LANE] * w2z[...], axis=0, keepdims=True)
                zbuf[par, zpos, b, 2 * n + h:2 * n + h + 1, :] = part

    def hidden_start(b, off):
        for n in range(rows // 256):
            abuf[b, :, n * 256:(n + 1) * 256] = jnp.dot(wb[:, 0:tiles.lanes], xt[0:tiles.lanes, pl.ds(off + n * 256, 256)],
                                                        preferred_element_type=f32)

    def first_pass(slot, h):
        per = piece // 256
        hidden_block(0, slot, pl.multiple_of(slot * rows, rows), h * per, (h + 1) * per)

    def take(slot, h):
        turn(slot, h)
        first_pass(slot, h)

    w2z[...] = jnp.where(rowid >= cut, w2b[...], 0.0)
    for h in range(parts):
        s0.landed(h)
        s2.start(h)
        s5.start(h)
    for h in range(parts):
        take(par_slot, h)
        first_pass(own_slot, h)
    for h in range(parts):
        s1.landed(h)
        s3.start(h)
        take(2 * down + q, h)
    for h in range(parts):
        s4.landed(h)
        take(2 * up + q, h)
    for h in range(parts):
        s5.landed(h)
        s6.start(h)
        take(2 * up + (1 - q), h)
    for h in range(parts):
        s2.landed(h)
        take(2 * down + (1 - q), h)
    for h in range(parts):
        s3.landed(h)
        take(2 * far + q, h)
        s6.landed(h)
        take(2 * far + (1 - q), h)

    def z_copy(par, g, d):
        block = pl.ds(blocks[g][0], sizes[g])
        return remote(zbuf.at[par, zpos, block], zbuf.at[par, zpos, block],
                      zsend.at[par, g, d], zrecv.at[par, g, d], zpeer[d])

    def r_copy(p, d):
        return remote(gsend[p].at[(rpos + d) % side], rsum[p].at[rpos], rsend.at[p, d], rrecv.at[p, d], rpeer[d])

    def a_copy(p, d):
        return remote(wag[p].at[rpos], wag[p].at[rpos], asend.at[p, d], arecv.at[p, d], rpeer[d])

    def fin_ring(arr, d):
        return remote(fin.at[arr, q, zpos, rpos], fin.at[arr, q, zpos, rpos], fsend.at[arr, d], frecv.at[arr, d], rpeer[d])

    def fin_cross(arr, e, d):
        block = fin.at[arr, q, zpos, (rpos + e) % side]
        return remote(block, block, csend.at[arr, e, d], crecv.at[arr, e, d], zpeer[d])

    def fin_pair(arr, w):
        block = fin.at[arr, q, (zpos + w) % side]
        return remote(block, block, psend.at[arr, w], precv.at[arr, w], partner)

    def spread(arr):
        for d in order:
            fin_ring(arr, d).start()
        for d in order:
            fin_cross(arr, 0, d).start()

    def relay(arr):
        for d in reversed(order):
            fin_ring(arr, d).wait_recv()
            for dd in order:
                fin_cross(arr, side - d, dd).start()

    def over(arr):
        fin_pair(arr, 0).start()
        for w in reversed(order):
            for e in range(side):
                fin_cross(arr, e, side - w).wait_recv()
            fin_pair(arr, w).start()

    for g in range(groups):
        for d in order:
            z_copy(0, g, d).start()
    for ship in (s0, s1, s2, s3, s4, s5, s6):
        ship.sent()

    def squares(main, out):
        low = cut // 8
        sq = jnp.zeros((8, LANE), f32)
        for p in range(2):
            n = tiles.count[p]
            wide = len({k for i, k in tiles.part[p] if i is not None})
            mains = tiles.nrow * wide
            for j in range(n):
                t = n * rpos + j
                v = main[span[p].start + 8 * j:span[p].start + 8 * j + 8, :]
                tile_row = jnp.where(t < mains, t // wide + 0 * lane8, (t - mains) * tiles.per + lane8 // rem)
                sq = sq + jnp.where(tile_row >= low, v * v, 0.0)
        for i in range(tiles.nrow):
            v = out[8 * i:8 * i + 8, :]
            sq = sq + jnp.where((i >= low) & (rpos == 0) & (lane8 == 0), v * v, 0.0)
        return sq

    def gradient(k, _):
        par = k % 2

        def weigh(g):
            for d in range(1, side):
                z_copy(par, g, d).wait_recv()
            for bb, b in enumerate(blocks[g]):
                logit = zbuf[par, 0, b]
                for s in range(1, side):
                    logit = logit + zbuf[par, s, b]
                ztot[b] = logit
                res = ybuf[b].astype(f32) - jax.nn.sigmoid(logit)
                for n in range(nlt):
                    act = abuf[b, :, n * LANE:(n + 1) * LANE]
                    rr = jnp.broadcast_to(res[n:n + 1, :], (hs, LANE))
                    part = rr * act
                    g2acc[...] = part if b == 0 and n == 0 else g2acc[...] + part
                    bbuf[bb, :, n * LANE:(n + 1) * LANE] = ((rr * w2b[...]) * (1.0 - act * act)).astype(bf16)

        def contract(g, first, last):
            for bb, b in enumerate(blocks[g]):
                for lo in range(first, last, 256):
                    hi = min(lo + 256, last)
                    prod = jnp.dot(bbuf[bb], x[b * rows:(b + 1) * rows, lo:hi], preferred_element_type=f32)
                    gacc[:, lo:hi] = prod if b == 0 else gacc[:, lo:hi] + prod

        for g in range(groups - 1):
            weigh(g)
            contract(g, 0, kpad)
        weigh(groups - 1)
        contract(groups - 1, 0, tiles.lanes)
        pack(0, gacc)
        for d in order:
            r_copy(0, d).start()
        contract(groups - 1, tiles.lanes, kpad)
        g2 = jnp.zeros((8, LANE), f32)
        for i in range(hs // 8):
            col = jnp.sum(g2acc[i * 8:(i + 1) * 8, :], axis=1, keepdims=True)
            g2 = jnp.where(lane8 == i, jnp.broadcast_to(col, (8, LANE)), g2)
        for o in range(side):
            gsend_b[o, size_b:size_b + 8, :] = g2
        pack(1, gacc)
        for d in order:
            r_copy(1, d).start()
        for p in range(2):
            rsum[p][rpos] = gsend[p][rpos]
        for g in range(groups):
            for d in range(1, side):
                z_copy(par, g, d).wait_send()
        coef = jnp.where((k == 0) | (k == LEAPS), 0.5 * step, step).astype(f32)

        def kick(p):
            for d in range(1, side):
                r_copy(p, d).wait_recv()
            total = rsum[p][0]
            for s in range(1, side):
                total = total + rsum[p][s]
            mom[span[p], :] = mom[span[p], :] + coef * (total[0:tiles.size[p]] - pos[span[p], :] / PRIOR_VAR)
            if p == 1:
                g2sum[...] = total[size_b:size_b + 8]

        def kick_out():
            tile = g2sum[...]
            for i in range(hs // 8):
                blk = slice(i * 8, (i + 1) * 8)
                gcol = jnp.broadcast_to(tile[:, i:i + 1], (8, LANE))
                m2b[blk, :] = m2b[blk, :] + coef * (gcol - w2b[blk, :] / PRIOR_VAR)

        @pl.when(k < LEAPS)
        def _():
            for p in range(2):
                kick(p)
                pos[span[p], :] = pos[span[p], :] + step * mom[span[p], :]
                wag[p][rpos] = pos[span[p], :].astype(bf16)
                for d in order:
                    a_copy(p, d).start()
            kick_out()
            w2b[...] = w2b[...] + step * m2b[...]
            w2z[...] = jnp.where(rowid >= cut, w2b[...], 0.0)

            @pl.when(k == LEAPS - 1)
            def _():
                fin[0, q, zpos, rpos, 0:urows, :] = pos[...]
                fin[0, q, zpos, rpos, urows:urows + 8, :] = jnp.zeros((8, LANE), f32)
                spread(0)

            for p in range(2):
                for d in range(1, side):
                    r_copy(p, d).wait_send()
            for p in range(2):
                for d in range(1, side):
                    a_copy(p, d).wait_recv()
                adopt(p, wag[p])
                if p == 0:
                    for b in blocks[0]:
                        hidden_start(b, b * rows)
            for g in range(groups):
                for b in blocks[g]:
                    hidden_block(1 - par, b, b * rows, 0, rows // 256, tiles.lanes if g == 0 else 0)
                for d in order:
                    z_copy(1 - par, g, d).start()
            for p in range(2):
                for d in range(1, side):
                    a_copy(p, d).wait_send()

            @pl.when(k == LEAPS - 1)
            def _():
                relay(0)

        @pl.when(k == LEAPS)
        def _():
            loss = jnp.zeros((8, LANE), f32)
            for b in range(nshard):
                zt = ztot[b]
                loss = loss + (jnp.maximum(zt, 0.0) + jnp.log1p(jnp.exp(-jnp.abs(zt))) - ybuf[b].astype(f32) * zt)
            estage[...] = jnp.where(zpos == 0, loss, 0.0) + squares(pos, w2b) / (2.0 * PRIOR_VAR)
            for p in range(2):
                kick(p)
            kick_out()
            for p in range(2):
                for d in range(1, side):
                    r_copy(p, d).wait_send()

        return 0

    lax.fori_loop(0, LEAPS + 1, gradient, 0)

    def as_row(ref):
        diag = jnp.where(rowid == lax.broadcasted_iota(jnp.int32, (hs, LANE), 1), ref[...], 0.0)
        return jnp.broadcast_to(jnp.sum(diag, axis=0, keepdims=True), (8, LANE))

    share = jnp.sum(estage[...] + 0.5 * squares(mom, m2b), axis=0, keepdims=True)
    misc = jnp.where(sub8 == 0, as_row(w2b), jnp.where(sub8 == 1, as_row(m2b), jnp.broadcast_to(share, (8, LANE))))

    fin[1, q, zpos, rpos, 0:urows, :] = mom[...]
    fin[1, q, zpos, rpos, urows:urows + 8, :] = misc
    spread(1)
    over(0)
    relay(1)
    over(1)
    for arr in range(2):
        for w in range(side):
            fin_pair(arr, w).wait()
        for d in order:
            fin_ring(arr, d).wait_send()
            for e in range(side):
                fin_cross(arr, e, d).wait_send()


def _unpack(cfg, fin, end_w, end_m, w_out, m_out, e_out, obuf, w_row, m_row, energy, sem, tail):
    side, hidden, feat, rows, hs, step, sizes = cfg
    chains = fin.shape[1]
    tiles = Tiles(side, feat, hs)
    base = (0, tiles.size[0])
    urows = tiles.size[0] + tiles.size[1]
    f32 = jnp.float32
    width = -(-hidden // LANE) * LANE
    lane = lax.broadcasted_iota(jnp.int32, (8, width), 1)
    for ch in range(chains):
        acc = jnp.zeros((8, width), f32)
        tot = jnp.zeros((8, LANE), f32)
        for z in range(side):
            tile = fin[1, ch, z, 0, urows:urows + 8, :]
            wide = jnp.concatenate([tile, jnp.zeros((8, width - LANE), f32)], axis=1)
            r0 = min(z * hs, hidden - hs)
            wide = pltpu.roll(wide, r0, 1) if r0 else wide
            acc = jnp.where((lane >= z * hs) & (lane < (z + 1) * hs), wide, acc)
            for r in range(side):
                tot = tot + fin[1, ch, z, r, urows:urows + 8, :]
        w_row[ch:ch + 1, :] = acc[0:1, 0:hidden]
        m_row[ch:ch + 1, :] = acc[1:2, 0:hidden]
        energy[ch] = jnp.sum(tot[2:3, :])
    copies = [pltpu.make_async_copy(src, dst, tail.at[i]) for i, (src, dst) in enumerate(((w_row, w_out), (m_row, m_out), (energy, e_out)))]
    for cp in copies:
        cp.start()
    for arr, ref in ((0, end_w), (1, end_m)):
        for ch in range(chains):
            for z in range(side):
                r0 = min(z * hs, hidden - hs)
                for p in range(2):
                    n = tiles.count[p]
                    for t, (i, k) in enumerate(tiles.part[p]):
                        at = base[p] + 8 * (t % n)
                        tile = fin[arr, ch, z, t // n, at:at + 8, :]
                        if i is not None:
                            obuf[arr, ch, r0 + 8 * i:r0 + 8 * i + 8, k * LANE:(k + 1) * LANE] = tile
                            continue
                        for g in range(min(tiles.per, tiles.nrow - k * tiles.per)):
                            r1 = r0 + 8 * (k * tiles.per + g)
                            v = pltpu.roll(tile, LANE - g * tiles.rem, 1) if g else tile
                            obuf[arr, ch, r1:r1 + 8, tiles.nfull * LANE:feat] = v[:, 0:tiles.rem]
            cp = pltpu.make_async_copy(obuf.at[arr, ch], ref.at[ch], sem.at[arr, ch])
            cp.start()
            copies.append(cp)
    for cp in copies:
        cp.wait()


def solution(mesh):
    row_spec = P('data', None)
    label_spec = P('data')
    in_spec = P(None, 'parts', None)
    out_spec = P('parts', None)
    chain_spec = P('parts')
    side = math.isqrt(mesh.shape['data'] // 2)

    def run_chains(feats, labels, w_in, w_out, mom_in, mom_out):
        num_rows, feat = feats.shape
        hidden = w_in.shape[2]
        step = 1.0 / math.sqrt(num_rows * (feat + hidden))

        def device_body(x_rows, y_rows, pos_in, pos_out, vel_in, vel_out):
            rows = x_rows.shape[0]
            chains = pos_out.shape[0]
            hs = -(-(hidden // 8) // side) * 8
            kpad = -(-feat // LANE) * LANE
            nshard = 2 * side
            size_a, size_b = Tiles(side, feat, hs).size
            urows = size_a + size_b
            sizes = (2, 3, 3)
            pieces = 4
            groups = len(sizes)
            f32, bf16 = jnp.float32, jnp.bfloat16
            dma = pltpu.SemaphoreType.DMA
            vm = pltpu.VMEM
            cfg = (side, hidden, feat, rows, hs, step, sizes)
            full = jax.ShapeDtypeStruct((chains, hidden, feat), f32)
            any_spec = pl.BlockSpec(memory_space=pl.ANY)
            vmem_spec = pl.BlockSpec(memory_space=pltpu.VMEM)
            hbm_spec = pl.BlockSpec(memory_space=pltpu.HBM)
            piece_shape = (2, chains, side, side, urows + 8, LANE)
            fin = pl.pallas_call(
                functools.partial(_kernel, cfg),
                out_shape=vm(piece_shape, f32),
                in_specs=[hbm_spec] * 6,
                out_specs=vmem_spec,
                scratch_shapes=[
                    vm((kpad, nshard * rows), bf16),
                    vm((nshard * rows, kpad), bf16),
                    vm((nshard, 8, rows // 8), jnp.int32),
                    vm((2, chains, hidden), f32),
                    vm((8, LANE), f32),
                    vm((8, LANE), f32),
                    vm((2, hs, feat), f32),
                    vm((hs, kpad), bf16),
                    vm((nshard, hs, rows), f32),
                    vm((max(sizes), hs, rows), bf16),
                    vm((hs, kpad), f32),
                    vm((hs, LANE), f32),
                    vm((side, size_a, LANE), f32),
                    vm((side, size_b + 8, LANE), f32),
                    vm((side, size_a, LANE), f32),
                    vm((side, size_b + 8, LANE), f32),
                    vm((urows, LANE), f32),
                    vm((urows, LANE), f32),
                    vm((hs, LANE), f32),
                    vm((hs, LANE), f32),
                    vm((hs, LANE), f32),
                    vm((side, size_a, LANE), bf16),
                    vm((side, size_b, LANE), bf16),
                    vm((2, side, nshard, 8, LANE), f32),
                    vm((nshard, 8, LANE), f32),
                    dma((2 + pieces,)), dma((7, pieces)), dma((7, pieces)), dma((8,)), dma((9,)),
                    dma((2, groups, side)), dma((2, groups, side)),
                    dma((2, side)), dma((2, side)), dma((2, side)), dma((2, side)),
                    dma((2, side)), dma((2, side)), dma((2, side, side)), dma((2, side, side)),
                    dma((2, side)), dma((2, side)),
                ],
                compiler_params=pltpu.CompilerParams(collective_id=0, has_side_effects=True, vmem_limit_bytes=67043328 - 4 * math.prod(piece_shape)),
            )(x_rows.T, y_rows.reshape(8, rows // 8), pos_in.transpose(1, 2, 0), vel_in.transpose(1, 2, 0), pos_out, vel_out)
            end_w, end_m, w_row, m_row, energy = pl.pallas_call(
                functools.partial(_unpack, cfg),
                out_shape=(full, full, jax.ShapeDtypeStruct((chains, hidden), f32), jax.ShapeDtypeStruct((chains, hidden), f32),
                           jax.ShapeDtypeStruct((chains,), f32)),
                in_specs=[vmem_spec],
                out_specs=(any_spec,) * 5,
                scratch_shapes=[vm((2, chains, hidden, feat), f32), vm((chains, hidden), f32), vm((chains, hidden), f32),
                                pltpu.SMEM((chains,), f32), dma((2, chains)), dma((3,))],
                compiler_params=pltpu.CompilerParams(vmem_limit_bytes=16 << 20),
            )(fin)
            return end_w.transpose(2, 0, 1), w_row, end_m.transpose(2, 0, 1), m_row, energy

        mapped = jax.shard_map(device_body, mesh=mesh, in_specs=(row_spec, label_spec, in_spec, out_spec, in_spec, out_spec), out_specs=(in_spec, out_spec, in_spec, out_spec, chain_spec), check_vma=False)
        return mapped(feats, labels, w_in, w_out, mom_in, mom_out)

    return run_chains
```

```python
import functools
import math

import jax
import jax.numpy as jnp
from jax import lax
from jax.experimental import pallas as pl
from jax.experimental.pallas import tpu as pltpu
from jax.sharding import PartitionSpec as P

LEAPS = 16
PRIOR_VAR = 1.0
LANE = 128
BEGIN = 6
MESH_ID = pl.DeviceIdType.MESH


class Tiles:
    def __init__(self, side, feat, hs):
        self.nrow = hs // 8
        self.nfull = feat // LANE
        self.rem = feat - self.nfull * LANE
        self.per = LANE // self.rem
        split = 2 * (self.nfull // 3)
        self.lanes = split * LANE
        left = [(None, j) for j in range(-(-self.nrow // self.per))]
        self.part = [[(i, k) for i in range(self.nrow) for k in range(split)],
                     [(i, k) for i in range(self.nrow) for k in range(split, self.nfull)] + left]
        self.count = [len(p) // side for p in self.part]
        assert all(len(p) % side == 0 for p in self.part)
        self.size = [8 * n for n in self.count]

    def value(self, src, tile):
        i, k = tile
        if i is not None:
            return src[8 * i:8 * i + 8, k * LANE:(k + 1) * LANE]
        acc = None
        for g in range(min(self.per, self.nrow - k * self.per)):
            i = k * self.per + g
            v = src[8 * i:8 * i + 8, self.nfull * LANE:src.shape[1]]
            if v.shape[1] < LANE:
                v = jnp.concatenate([v, jnp.zeros((8, LANE - v.shape[1]), v.dtype)], axis=1)
                v = pltpu.roll(v, g * self.rem, 1) if g else v
            else:
                v = jnp.where(self.group() == g, v, 0.0)
            acc = v if acc is None else acc + v
        return acc

    def group(self):
        return lax.broadcasted_iota(jnp.int32, (8, LANE), 1) // self.rem


def _kernel(cfg, xt_hbm, lab_hbm, w_hbm, m_hbm, wo_hbm, mo_hbm, fin,
            xt, x, ybuf, oload, estage, g2sum, wload, wb, abuf, bbuf, gacc, g2acc, gsend_a, gsend_b, rsum_a, rsum_b, pos, mom, w2b, m2b, w2z,
            wag_a, zbuf, ztot,
            lsem, isend, irecv, ysend, yrecv, zsend, zrecv, rsend, rrecv, asend, arecv, fsend, frecv,
            csend, crecv, psend, precv):
    side, hidden, feat, rows, hs, step, sizes = cfg
    half = side // 2
    nshard = 2 * side
    tiles = Tiles(side, feat, hs)
    nfull, rem = tiles.nfull, tiles.rem
    size_a, size_b = tiles.size
    urows = size_a + size_b
    full_b = side * size_b
    span = (slice(0, size_a), slice(size_a, size_a + full_b))
    kpad = xt.shape[0]
    nlt = rows // LANE
    begin = BEGIN
    groups = len(sizes)
    blocks = [range(sum(sizes[:g]), sum(sizes[:g + 1])) for g in range(groups)]
    f32, bf16 = jnp.float32, jnp.bfloat16

    me = lax.axis_index('data')
    core = me % 2
    xx = (me // 2) % side
    yy = me // (2 * side)

    def fold(y, x_):
        return (x_ // half + y // half) % 2

    q = (core + fold(yy, xx)) % 2
    zpos = xx * (1 - q) + yy * q
    rpos = yy * (1 - q) + xx * q

    def device(z, r, role):
        x2 = z * (1 - role) + r * role
        y2 = r * (1 - role) + z * role
        return {'data': (y2 * side + x2) * 2 + (role + fold(y2, x2)) % 2}

    zpeer = [device((zpos + d) % side, rpos, q) for d in range(side)]
    rpeer = [device(zpos, (rpos + d) % side, q) for d in range(side)]
    partner = device(rpos, zpos, 1 - q)

    def remote(src, dst, ssem, rsem, dev):
        return pltpu.make_async_remote_copy(src_ref=src, dst_ref=dst, send_sem=ssem, recv_sem=rsem,
                                            device_id=dev, device_id_type=MESH_ID)

    start = jnp.minimum(zpos * hs, hidden - hs)
    start = pl.multiple_of(start, 8)
    cut = zpos * hs - start

    own_slot = 2 * zpos + q
    par_slot = 2 * zpos + (1 - q)

    parts = isend.shape[1]
    piece = rows // parts
    order = [d for d in range(1, side) if d == half] + [d for d in range(1, side) if d != half]

    def xcols(slot, h):
        return xt.at[pl.ds(0, feat), pl.ds(pl.multiple_of(slot * rows + h * piece, piece), piece)]

    load_x = [pltpu.make_async_copy(xt_hbm.at[:, pl.ds(h * piece, piece)], xcols(own_slot, h), lsem.at[2 + h]) for h in range(parts)]
    load_w = pltpu.make_async_copy(w_hbm.at[q, pl.ds(start, hs), :], wload.at[0], lsem.at[0])
    load_m = pltpu.make_async_copy(m_hbm.at[q, pl.ds(start, hs), :], wload.at[1], lsem.at[1])
    load_y = pltpu.make_async_copy(lab_hbm, ybuf.at[own_slot], ysend.at[7])
    load_o = [pltpu.make_async_copy(src, oload.at[i], yrecv.at[7 + i]) for i, src in enumerate((wo_hbm, mo_hbm))]
    for cp in load_x + [load_y, load_w, load_m] + load_o:
        cp.start()

    barrier = pltpu.get_barrier_semaphore()
    for dev in zpeer[1:] + rpeer[1:] + [partner]:
        pl.semaphore_signal(barrier, inc=1, device_id=dev, device_id_type=MESH_ID)
    pl.semaphore_wait(barrier, 2 * side - 1)

    class Ship:
        def __init__(self, i, slot, dslot, dev):
            self.x = [remote(xcols(slot, h), xcols(dslot, h), isend.at[i, h], irecv.at[i, h], dev) for h in range(parts)]
            self.y = remote(ybuf.at[slot], ybuf.at[dslot], ysend.at[i], yrecv.at[i], dev)

        def start(self, h):
            self.x[h].start()
            if h == parts - 1:
                self.y.start()

        def landed(self, h):
            self.x[h].wait_recv()
            if h == parts - 1:
                self.y.wait_recv()

        def sent(self):
            for c in self.x:
                c.wait_send()
            self.y.wait_send()

    def turn(slot, h):
        def body(t, _):
            off = pl.multiple_of(slot * rows + h * piece + t * LANE, LANE)
            for row in range(feat, kpad, rem):
                xt[row:row + rem, pl.ds(off, LANE)] = xt[feat - rem:feat, pl.ds(off, LANE)]
            x[pl.ds(off, LANE), :] = xt[:, pl.ds(off, LANE)].T
            return 0
        lax.fori_loop(0, piece // LANE, body, 0)

    up, down, far = (zpos + 1) % side, (zpos + side - 1) % side, (zpos + 2) % side
    forth, back = zpeer[1], zpeer[side - 1]
    s0 = Ship(0, own_slot, 2 * rpos + q, partner)
    s1 = Ship(1, own_slot, own_slot, forth)
    s2 = Ship(2, par_slot, par_slot, forth)
    s3 = Ship(3, 2 * down + q, 2 * down + q, forth)
    s4 = Ship(4, own_slot, own_slot, back)
    s5 = Ship(5, par_slot, par_slot, back)
    s6 = Ship(6, 2 * up + (1 - q), 2 * up + (1 - q), back)
    load_y.wait()
    for h in range(parts):
        load_x[h].wait()
        for ship in (s0, s1, s4):
            ship.start(h)
    for h in range(parts):
        turn(own_slot, h)

    lane8 = lax.broadcasted_iota(jnp.int32, (8, LANE), 1)
    sub8 = lax.broadcasted_iota(jnp.int32, (8, LANE), 0)

    def pack(p, src):
        n = tiles.count[p]
        for t, tile in enumerate(tiles.part[p]):
            if p == 0:
                gsend_a[t // n, 8 * (t % n):8 * (t % n) + 8, :] = tiles.value(src, tile)
            else:
                gsend_b[8 * t:8 * t + 8, :] = tiles.value(src, tile)

    def adopt(p, src):
        n = tiles.count[p]
        if p == 0:
            held = [src[o].astype(f32) for o in range(side)]
            got = {tile: held[t // n][8 * (t % n):8 * (t % n) + 8] for t, tile in enumerate(tiles.part[p])}
        else:
            got = {tile: src[size_a + 8 * t:size_a + 8 * t + 8, :] for t, tile in enumerate(tiles.part[p])}
        for k in sorted({k for i, k in tiles.part[p] if i is not None}):
            for i in range(0, tiles.nrow, 2):
                v = got[i, k] if i + 1 == tiles.nrow else jnp.concatenate([got[i, k], got[i + 1, k]], axis=0)
                wb[8 * i:8 * i + v.shape[0], k * LANE:(k + 1) * LANE] = v.astype(bf16)
        if (None, 0) in got:
            def left(i):
                return jnp.where(tiles.group() == i % tiles.per, got[None, i // tiles.per], 0.0)
            for i in range(0, tiles.nrow, 2):
                v = left(i) if i + 1 == tiles.nrow else jnp.concatenate([left(i), left(i + 1)], axis=0)
                wb[8 * i:8 * i + v.shape[0], nfull * LANE:] = v.astype(bf16)

    load_w.wait()
    load_m.wait()
    for src, dst in ((1, mom), (0, pos)):
        for p in range(2):
            pack(p, wload.at[src])
        dst[span[0], :] = gsend_a[rpos]
        dst[span[1], :] = gsend_b[0:full_b]
    adopt(0, gsend_a)
    adopt(1, pos)

    def column(ref, dst):
        width = -(-hidden // LANE) * LANE
        v = jnp.concatenate([oload[ref, pl.ds(q, 1), :], jnp.zeros((1, width - hidden), f32)], axis=1)
        lanes = lax.broadcasted_iota(jnp.int32, (8, width), 1)
        subs = lax.broadcasted_iota(jnp.int32, (8, width), 0)
        v = jnp.broadcast_to(v, (8, width))
        for i in range(hs // 8):
            hit = jnp.where(lanes == start + i * 8 + subs, v, 0.0)
            dst[i * 8:(i + 1) * 8, :] = jnp.broadcast_to(jnp.sum(hit, axis=1, keepdims=True), (8, LANE))

    for cp in load_o:
        cp.wait()
    column(0, w2b)
    column(1, m2b)

    rowid = lax.broadcasted_iota(jnp.int32, (hs, LANE), 0)

    split = tiles.lanes

    def hidden_block(par, b, off, first, last, begun=False):
        for n in range(first, last):
            cols = pl.ds(off + n * 256, 256)
            if begun:
                pre = jnp.dot(wb[:, 0:split], xt[0:split, cols], preferred_element_type=f32) + abuf[b, :, n * 256:(n + 1) * 256]
            else:
                pre = jnp.dot(wb[...], xt[:, cols], preferred_element_type=f32)
            act = jnp.tanh(pre)
            abuf[b, :, n * 256:(n + 1) * 256] = act
            for h in range(2):
                part = jnp.sum(act[:, h * LANE:(h + 1) * LANE] * w2z[...], axis=0, keepdims=True)
                zbuf[par, zpos, b, 2 * n + h:2 * n + h + 1, :] = part

    def hidden_start(b, off):
        for n in range(rows // 256):
            abuf[b, :, n * 256:(n + 1) * 256] = jnp.dot(wb[:, split:], xt[split:, pl.ds(off + n * 256, 256)],
                                                        preferred_element_type=f32)

    def first_pass(slot, h):
        per = piece // 256
        hidden_block(0, slot, pl.multiple_of(slot * rows, rows), h * per, (h + 1) * per)

    def take(slot, h):
        turn(slot, h)
        first_pass(slot, h)

    w2z[...] = jnp.where(rowid >= cut, w2b[...], 0.0)
    for h in range(parts):
        s0.landed(h)
        s2.start(h)
        s5.start(h)
    for h in range(parts):
        take(par_slot, h)
        first_pass(own_slot, h)
    for h in range(parts):
        s1.landed(h)
        s3.start(h)
        take(2 * down + q, h)
    for h in range(parts):
        s4.landed(h)
        take(2 * up + q, h)
    for h in range(parts):
        s5.landed(h)
        s6.start(h)
        take(2 * up + (1 - q), h)
    for h in range(parts):
        s2.landed(h)
        take(2 * down + (1 - q), h)
    for h in range(parts):
        s3.landed(h)
        take(2 * far + q, h)
        s6.landed(h)
        take(2 * far + (1 - q), h)

    def z_copy(par, g, d):
        block = pl.ds(blocks[g][0], sizes[g])
        return remote(zbuf.at[par, zpos, block], zbuf.at[par, zpos, block],
                      zsend.at[par, g, d], zrecv.at[par, g, d], zpeer[d])

    def r_copy(p, d, par):
        if p == 0:
            return remote(gsend_a.at[(rpos + d) % side], rsum_a.at[rpos], rsend.at[0, d], rrecv.at[0, d], rpeer[d])
        return remote(gsend_b, rsum_b.at[par, rpos], rsend.at[1 + par, d], rrecv.at[1 + par, d], rpeer[d])

    def a_copy(d):
        return remote(wag_a.at[rpos], wag_a.at[rpos], asend.at[d], arecv.at[d], rpeer[d])

    def own_share():
        return pl.ds(pl.multiple_of(size_a + rpos * size_b, 8), size_b)

    def fin_ring(arr, d):
        return remote(fin.at[arr, q, zpos, rpos], fin.at[arr, q, zpos, rpos], fsend.at[arr, d], frecv.at[arr, d], rpeer[d])

    def fin_cross(arr, e, d):
        block = fin.at[arr, q, zpos, (rpos + e) % side]
        return remote(block, block, csend.at[arr, e, d], crecv.at[arr, e, d], zpeer[d])

    def fin_pair(arr, w):
        block = fin.at[arr, q, (zpos + w) % side]
        return remote(block, block, psend.at[arr, w], precv.at[arr, w], partner)

    def spread(arr):
        for d in order:
            fin_ring(arr, d).start()
        for d in order:
            fin_cross(arr, 0, d).start()

    def relay(arr):
        for d in reversed(order):
            fin_ring(arr, d).wait_recv()
            for dd in order:
                fin_cross(arr, side - d, dd).start()

    def over(arr):
        fin_pair(arr, 0).start()
        for w in reversed(order):
            for e in range(side):
                fin_cross(arr, e, side - w).wait_recv()
            fin_pair(arr, w).start()

    for g in range(groups):
        for d in order:
            z_copy(0, g, d).start()
    for ship in (s0, s1, s2, s3, s4, s5, s6):
        ship.sent()

    def squares(main, out):
        low = cut // 8
        sq = jnp.zeros((8, LANE), f32)
        for p in range(2):
            n = tiles.count[p]
            wide = len({k for i, k in tiles.part[p] if i is not None})
            mains = tiles.nrow * wide
            for j in range(n):
                t = n * rpos + j
                at = 8 * j if p == 0 else pl.multiple_of(size_a + 8 * (n * rpos + j), 8)
                v = main[pl.ds(at, 8), :]
                tile_row = jnp.where(t < mains, t // wide + 0 * lane8, (t - mains) * tiles.per + lane8 // rem)
                sq = sq + jnp.where(tile_row >= low, v * v, 0.0)
        for i in range(tiles.nrow):
            v = out[8 * i:8 * i + 8, :]
            sq = sq + jnp.where((i >= low) & (rpos == 0) & (lane8 == 0), v * v, 0.0)
        return sq

    def gradient(k, _):
        par = k % 2

        def weigh(g):
            for d in range(1, side):
                z_copy(par, g, d).wait_recv()
            for b in blocks[g]:
                logit = zbuf[par, 0, b]
                for s in range(1, side):
                    logit = logit + zbuf[par, s, b]
                ztot[b] = logit
                res = ybuf[b].astype(f32) - jax.nn.sigmoid(logit)
                for n in range(nlt):
                    act = abuf[b, :, n * LANE:(n + 1) * LANE]
                    rr = jnp.broadcast_to(res[n:n + 1, :], (hs, LANE))
                    part = rr * act
                    g2acc[...] = part if b == 0 and n == 0 else g2acc[...] + part
                    bbuf[b, :, n * LANE:(n + 1) * LANE] = ((rr * w2b[...]) * (1.0 - act * act)).astype(bf16)

        def contract(g, first, last):
            for b in blocks[g]:
                for lo in range(first, last, 256):
                    hi = min(lo + 256, last)
                    prod = jnp.dot(bbuf[b], x[b * rows:(b + 1) * rows, lo:hi], preferred_element_type=f32)
                    gacc[:, lo:hi] = prod if b == 0 else gacc[:, lo:hi] + prod

        for g in range(groups):
            weigh(g)
            contract(g, 0, split)
        pack(0, gacc)
        for d in order:
            r_copy(0, d, par).start()
        g2 = jnp.zeros((8, LANE), f32)
        for i in range(hs // 8):
            col = jnp.sum(g2acc[i * 8:(i + 1) * 8, :], axis=1, keepdims=True)
            g2 = jnp.where(lane8 == i, jnp.broadcast_to(col, (8, LANE)), g2)
        gsend_b[full_b:full_b + 8, :] = g2
        for g in range(groups):
            contract(g, split, kpad)
        pack(1, gacc)
        for d in order:
            r_copy(1, d, par).start()
        rsum_a[rpos] = gsend_a[rpos]
        rsum_b[par, rpos] = gsend_b[...]
        for g in range(groups):
            for d in range(1, side):
                z_copy(par, g, d).wait_send()
        coef = jnp.where((k == 0) | (k == LEAPS), 0.5 * step, step).astype(f32)

        def kick(p):
            for d in range(1, side):
                r_copy(p, d, par).wait_recv()
            held = [rsum_a[s] if p == 0 else rsum_b[par, s] for s in range(side)]
            total = held[0]
            for s in range(1, side):
                total = total + held[s]
            size = size_a if p == 0 else full_b
            mom[span[p], :] = mom[span[p], :] + coef * (total[0:size] - pos[span[p], :] / PRIOR_VAR)
            if p == 1:
                g2sum[...] = total[size:size + 8]

        def kick_out():
            tile = g2sum[...]
            for i in range(hs // 8):
                blk = slice(i * 8, (i + 1) * 8)
                gcol = jnp.broadcast_to(tile[:, i:i + 1], (8, LANE))
                m2b[blk, :] = m2b[blk, :] + coef * (gcol - w2b[blk, :] / PRIOR_VAR)

        @pl.when(k < LEAPS)
        def _():
            kick(0)
            pos[span[0], :] = pos[span[0], :] + step * mom[span[0], :]
            wag_a[rpos] = pos[span[0], :].astype(bf16)
            for d in order:
                a_copy(d).start()
            kick(1)
            pos[span[1], :] = pos[span[1], :] + step * mom[span[1], :]
            adopt(1, pos)
            for b in range(begin):
                hidden_start(b, b * rows)
            kick_out()
            w2b[...] = w2b[...] + step * m2b[...]
            w2z[...] = jnp.where(rowid >= cut, w2b[...], 0.0)

            @pl.when(k == LEAPS - 1)
            def _():
                fin[0, q, zpos, rpos, 0:size_a, :] = pos[span[0], :]
                fin[0, q, zpos, rpos, size_a:urows, :] = pos[own_share(), :]
                fin[0, q, zpos, rpos, urows:urows + 8, :] = jnp.zeros((8, LANE), f32)
                spread(0)

            for p in range(2):
                for d in range(1, side):
                    r_copy(p, d, par).wait_send()
            for d in range(1, side):
                a_copy(d).wait_recv()
            adopt(0, wag_a)
            for g in range(groups):
                for b in blocks[g]:
                    hidden_block(1 - par, b, b * rows, 0, rows // 256, b < begin)
                for d in order:
                    z_copy(1 - par, g, d).start()
            for d in range(1, side):
                a_copy(d).wait_send()

            @pl.when(k == LEAPS - 1)
            def _():
                relay(0)

        @pl.when(k == LEAPS)
        def _():
            loss = jnp.zeros((8, LANE), f32)
            for b in range(nshard):
                zt = ztot[b]
                loss = loss + (jnp.maximum(zt, 0.0) + jnp.log1p(jnp.exp(-jnp.abs(zt))) - ybuf[b].astype(f32) * zt)
            estage[...] = jnp.where(zpos == 0, loss, 0.0) + squares(pos, w2b) / (2.0 * PRIOR_VAR)
            for p in range(2):
                kick(p)
            kick_out()
            for p in range(2):
                for d in range(1, side):
                    r_copy(p, d, par).wait_send()

        return 0

    lax.fori_loop(0, LEAPS + 1, gradient, 0)

    def as_row(ref):
        diag = jnp.where(rowid == lax.broadcasted_iota(jnp.int32, (hs, LANE), 1), ref[...], 0.0)
        return jnp.broadcast_to(jnp.sum(diag, axis=0, keepdims=True), (8, LANE))

    share = jnp.sum(estage[...] + 0.5 * squares(mom, m2b), axis=0, keepdims=True)
    misc = jnp.where(sub8 == 0, as_row(w2b), jnp.where(sub8 == 1, as_row(m2b), jnp.broadcast_to(share, (8, LANE))))

    fin[1, q, zpos, rpos, 0:size_a, :] = mom[span[0], :]
    fin[1, q, zpos, rpos, size_a:urows, :] = mom[own_share(), :]
    fin[1, q, zpos, rpos, urows:urows + 8, :] = misc
    spread(1)
    over(0)
    relay(1)
    over(1)
    for arr in range(2):
        for w in range(side):
            fin_pair(arr, w).wait()
        for d in order:
            fin_ring(arr, d).wait_send()
            for e in range(side):
                fin_cross(arr, e, d).wait_send()


def _unpack(cfg, fin, end_w, end_m, w_out, m_out, e_out, obuf, w_row, m_row, energy, sem, tail):
    side, hidden, feat, rows, hs, step, sizes = cfg
    chains = fin.shape[1]
    tiles = Tiles(side, feat, hs)
    base = (0, tiles.size[0])
    urows = tiles.size[0] + tiles.size[1]
    f32 = jnp.float32
    width = -(-hidden // LANE) * LANE
    lane = lax.broadcasted_iota(jnp.int32, (8, width), 1)
    for ch in range(chains):
        acc = jnp.zeros((8, width), f32)
        tot = jnp.zeros((8, LANE), f32)
        for z in range(side):
            tile = fin[1, ch, z, 0, urows:urows + 8, :]
            wide = jnp.concatenate([tile, jnp.zeros((8, width - LANE), f32)], axis=1)
            r0 = min(z * hs, hidden - hs)
            wide = pltpu.roll(wide, r0, 1) if r0 else wide
            acc = jnp.where((lane >= z * hs) & (lane < (z + 1) * hs), wide, acc)
            for r in range(side):
                tot = tot + fin[1, ch, z, r, urows:urows + 8, :]
        w_row[ch:ch + 1, :] = acc[0:1, 0:hidden]
        m_row[ch:ch + 1, :] = acc[1:2, 0:hidden]
        energy[ch] = jnp.sum(tot[2:3, :])
    copies = [pltpu.make_async_copy(src, dst, tail.at[i]) for i, (src, dst) in enumerate(((w_row, w_out), (m_row, m_out), (energy, e_out)))]
    for cp in copies:
        cp.start()
    for arr, ref in ((0, end_w), (1, end_m)):
        for ch in range(chains):
            for z in range(side):
                r0 = min(z * hs, hidden - hs)
                for p in range(2):
                    n = tiles.count[p]
                    for t, (i, k) in enumerate(tiles.part[p]):
                        at = base[p] + 8 * (t % n)
                        tile = fin[arr, ch, z, t // n, at:at + 8, :]
                        if i is not None:
                            obuf[arr, ch, r0 + 8 * i:r0 + 8 * i + 8, k * LANE:(k + 1) * LANE] = tile
                            continue
                        for g in range(min(tiles.per, tiles.nrow - k * tiles.per)):
                            r1 = r0 + 8 * (k * tiles.per + g)
                            v = pltpu.roll(tile, LANE - g * tiles.rem, 1) if g else tile
                            obuf[arr, ch, r1:r1 + 8, tiles.nfull * LANE:feat] = v[:, 0:tiles.rem]
            cp = pltpu.make_async_copy(obuf.at[arr, ch], ref.at[ch], sem.at[arr, ch])
            cp.start()
            copies.append(cp)
    for cp in copies:
        cp.wait()


def solution(mesh):
    row_spec = P('data', None)
    label_spec = P('data')
    in_spec = P(None, 'parts', None)
    out_spec = P('parts', None)
    chain_spec = P('parts')
    side = math.isqrt(mesh.shape['data'] // 2)

    def run_chains(feats, labels, w_in, w_out, mom_in, mom_out):
        num_rows, feat = feats.shape
        hidden = w_in.shape[2]
        step = 1.0 / math.sqrt(num_rows * (feat + hidden))

        def device_body(x_rows, y_rows, pos_in, pos_out, vel_in, vel_out):
            rows = x_rows.shape[0]
            chains = pos_out.shape[0]
            hs = -(-(hidden // 8) // side) * 8
            kpad = -(-feat // LANE) * LANE
            nshard = 2 * side
            size_a, size_b = Tiles(side, feat, hs).size
            urows = size_a + size_b
            sizes = (3, 3, 2)
            pieces = 4
            groups = len(sizes)
            f32, bf16 = jnp.float32, jnp.bfloat16
            dma = pltpu.SemaphoreType.DMA
            vm = pltpu.VMEM
            cfg = (side, hidden, feat, rows, hs, step, sizes)
            full = jax.ShapeDtypeStruct((chains, hidden, feat), f32)
            any_spec = pl.BlockSpec(memory_space=pl.ANY)
            vmem_spec = pl.BlockSpec(memory_space=pltpu.VMEM)
            hbm_spec = pl.BlockSpec(memory_space=pltpu.HBM)
            piece_shape = (2, chains, side, side, urows + 8, LANE)
            fin = pl.pallas_call(
                functools.partial(_kernel, cfg),
                out_shape=vm(piece_shape, f32),
                in_specs=[hbm_spec] * 6,
                out_specs=vmem_spec,
                scratch_shapes=[
                    vm((kpad, nshard * rows), bf16),
                    vm((nshard * rows, kpad), bf16),
                    vm((nshard, 8, rows // 8), jnp.int32),
                    vm((2, chains, hidden), f32),
                    vm((8, LANE), f32),
                    vm((8, LANE), f32),
                    vm((2, hs, feat), f32),
                    vm((hs, kpad), bf16),
                    vm((nshard, hs, rows), f32),
                    vm((nshard, hs, rows), bf16),
                    vm((hs, kpad), f32),
                    vm((hs, LANE), f32),
                    vm((side, size_a, LANE), f32),
                    vm((side * size_b + 8, LANE), f32),
                    vm((side, size_a, LANE), f32),
                    vm((2, side, side * size_b + 8, LANE), f32),
                    vm((size_a + side * size_b, LANE), f32),
                    vm((size_a + side * size_b, LANE), f32),
                    vm((hs, LANE), f32),
                    vm((hs, LANE), f32),
                    vm((hs, LANE), f32),
                    vm((side, size_a, LANE), bf16),
                    vm((2, side, nshard, 8, LANE), f32),
                    vm((nshard, 8, LANE), f32),
                    dma((2 + pieces,)), dma((7, pieces)), dma((7, pieces)), dma((8,)), dma((9,)),
                    dma((2, groups, side)), dma((2, groups, side)),
                    dma((3, side)), dma((3, side)), dma((side,)), dma((side,)),
                    dma((2, side)), dma((2, side)), dma((2, side, side)), dma((2, side, side)),
                    dma((2, side)), dma((2, side)),
                ],
                compiler_params=pltpu.CompilerParams(collective_id=0, has_side_effects=True, vmem_limit_bytes=67043328 - 4 * math.prod(piece_shape)),
            )(x_rows.T, y_rows.reshape(8, rows // 8), pos_in.transpose(1, 2, 0), vel_in.transpose(1, 2, 0), pos_out, vel_out)
            end_w, end_m, w_row, m_row, energy = pl.pallas_call(
                functools.partial(_unpack, cfg),
                out_shape=(full, full, jax.ShapeDtypeStruct((chains, hidden), f32), jax.ShapeDtypeStruct((chains, hidden), f32),
                           jax.ShapeDtypeStruct((chains,), f32)),
                in_specs=[vmem_spec],
                out_specs=(any_spec,) * 5,
                scratch_shapes=[vm((2, chains, hidden, feat), f32), vm((chains, hidden), f32), vm((chains, hidden), f32),
                                pltpu.SMEM((chains,), f32), dma((2, chains)), dma((3,))],
                compiler_params=pltpu.CompilerParams(vmem_limit_bytes=16 << 20),
            )(fin)
            return end_w.transpose(2, 0, 1), w_row, end_m.transpose(2, 0, 1), m_row, energy

        mapped = jax.shard_map(device_body, mesh=mesh, in_specs=(row_spec, label_spec, in_spec, out_spec, in_spec, out_spec), out_specs=(in_spec, out_spec, in_spec, out_spec, chain_spec), check_vma=False)
        return mapped(feats, labels, w_in, w_out, mom_in, mom_out)

    return run_chains
```

```python
import functools
import math

import jax
import jax.numpy as jnp
from jax import lax
from jax.experimental import pallas as pl
from jax.experimental.pallas import tpu as pltpu
from jax.sharding import PartitionSpec as P

LEAPS = 16
PRIOR_VAR = 1.0
LANE = 128
BEGIN = 6
MESH_ID = pl.DeviceIdType.MESH


class Tiles:
    def __init__(self, side, feat, hs):
        self.nrow = hs // 8
        self.nfull = feat // LANE
        self.rem = feat - self.nfull * LANE
        self.per = LANE // self.rem
        split = 2 * (self.nfull // 3)
        self.lanes = split * LANE
        left = [(None, j) for j in range(-(-self.nrow // self.per))]
        self.part = [[(i, k) for i in range(self.nrow) for k in range(split)],
                     [(i, k) for i in range(self.nrow) for k in range(split, self.nfull)] + left]
        self.count = [len(p) // side for p in self.part]
        assert all(len(p) % side == 0 for p in self.part)
        self.size = [8 * n for n in self.count]

    def value(self, src, tile):
        i, k = tile
        if i is not None:
            return src[8 * i:8 * i + 8, k * LANE:(k + 1) * LANE]
        acc = None
        for g in range(min(self.per, self.nrow - k * self.per)):
            i = k * self.per + g
            v = src[8 * i:8 * i + 8, self.nfull * LANE:src.shape[1]]
            if v.shape[1] < LANE:
                v = jnp.concatenate([v, jnp.zeros((8, LANE - v.shape[1]), v.dtype)], axis=1)
                v = pltpu.roll(v, g * self.rem, 1) if g else v
            else:
                v = jnp.where(self.group() == g, v, 0.0)
            acc = v if acc is None else acc + v
        return acc

    def group(self):
        return lax.broadcasted_iota(jnp.int32, (8, LANE), 1) // self.rem


def _kernel(cfg, xt_hbm, lab_hbm, w_hbm, m_hbm, wo_hbm, mo_hbm, fin,
            xt, x, ybuf, oload, estage, g2sum, wload, wb, abuf, bbuf, gacc, g2acc, gsend_a, gsend_b, rsum_a, rsum_b, pos, mom, w2b, m2b, w2z,
            wag_a, zbuf, ztot,
            lsem, isend, irecv, ysend, yrecv, zsend, zrecv, rsend, rrecv, asend, arecv, fsend, frecv,
            csend, crecv, psend, precv):
    side, hidden, feat, rows, hs, step, sizes = cfg
    half = side // 2
    nshard = 2 * side
    tiles = Tiles(side, feat, hs)
    nfull, rem = tiles.nfull, tiles.rem
    size_a, size_b = tiles.size
    urows = size_a + size_b
    full_b = side * size_b
    head = size_a + 8
    span = (slice(0, size_a), slice(size_a, size_a + full_b))
    kpad = xt.shape[0]
    nlt = rows // LANE
    begin = BEGIN
    groups = len(sizes)
    blocks = [range(sum(sizes[:g]), sum(sizes[:g + 1])) for g in range(groups)]
    f32, bf16 = jnp.float32, jnp.bfloat16

    me = lax.axis_index('data')
    core = me % 2
    xx = (me // 2) % side
    yy = me // (2 * side)

    def fold(y, x_):
        return (x_ // half + y // half) % 2

    q = (core + fold(yy, xx)) % 2
    zpos = xx * (1 - q) + yy * q
    rpos = yy * (1 - q) + xx * q

    def device(z, r, role):
        x2 = z * (1 - role) + r * role
        y2 = r * (1 - role) + z * role
        return {'data': (y2 * side + x2) * 2 + (role + fold(y2, x2)) % 2}

    zpeer = [device((zpos + d) % side, rpos, q) for d in range(side)]
    rpeer = [device(zpos, (rpos + d) % side, q) for d in range(side)]
    partner = device(rpos, zpos, 1 - q)

    def remote(src, dst, ssem, rsem, dev):
        return pltpu.make_async_remote_copy(src_ref=src, dst_ref=dst, send_sem=ssem, recv_sem=rsem,
                                            device_id=dev, device_id_type=MESH_ID)

    start = jnp.minimum(zpos * hs, hidden - hs)
    start = pl.multiple_of(start, 8)
    cut = zpos * hs - start

    own_slot = 2 * zpos + q
    par_slot = 2 * zpos + (1 - q)

    parts = isend.shape[1]
    piece = rows // parts
    order = [d for d in range(1, side) if d == half] + [d for d in range(1, side) if d != half]

    def xcols(slot, h):
        return xt.at[pl.ds(0, feat), pl.ds(pl.multiple_of(slot * rows + h * piece, piece), piece)]

    load_x = [pltpu.make_async_copy(xt_hbm.at[:, pl.ds(h * piece, piece)], xcols(own_slot, h), lsem.at[2 + h]) for h in range(parts)]
    load_w = pltpu.make_async_copy(w_hbm.at[q, pl.ds(start, hs), :], wload.at[0], lsem.at[0])
    load_m = pltpu.make_async_copy(m_hbm.at[q, pl.ds(start, hs), :], wload.at[1], lsem.at[1])
    load_y = pltpu.make_async_copy(lab_hbm, ybuf.at[own_slot], ysend.at[7])
    load_o = [pltpu.make_async_copy(src, oload.at[i], yrecv.at[7 + i]) for i, src in enumerate((wo_hbm, mo_hbm))]
    for cp in load_x + [load_y, load_w, load_m] + load_o:
        cp.start()

    barrier = pltpu.get_barrier_semaphore()
    for dev in zpeer[1:] + rpeer[1:] + [partner]:
        pl.semaphore_signal(barrier, inc=1, device_id=dev, device_id_type=MESH_ID)
    pl.semaphore_wait(barrier, 2 * side - 1)

    class Ship:
        def __init__(self, i, slot, dslot, dev):
            self.x = [remote(xcols(slot, h), xcols(dslot, h), isend.at[i, h], irecv.at[i, h], dev) for h in range(parts)]
            self.y = remote(ybuf.at[slot], ybuf.at[dslot], ysend.at[i], yrecv.at[i], dev)

        def start(self, h):
            self.x[h].start()
            if h == parts - 1:
                self.y.start()

        def landed(self, h):
            self.x[h].wait_recv()
            if h == parts - 1:
                self.y.wait_recv()

        def sent(self):
            for c in self.x:
                c.wait_send()
            self.y.wait_send()

    def turn(slot, h):
        def body(t, _):
            off = pl.multiple_of(slot * rows + h * piece + t * LANE, LANE)
            for row in range(feat, kpad, rem):
                xt[row:row + rem, pl.ds(off, LANE)] = xt[feat - rem:feat, pl.ds(off, LANE)]
            x[pl.ds(off, LANE), :] = xt[:, pl.ds(off, LANE)].T
            return 0
        lax.fori_loop(0, piece // LANE, body, 0)

    up, down, far = (zpos + 1) % side, (zpos + side - 1) % side, (zpos + 2) % side
    forth, back = zpeer[1], zpeer[side - 1]
    s0 = Ship(0, own_slot, 2 * rpos + q, partner)
    s1 = Ship(1, own_slot, own_slot, forth)
    s2 = Ship(2, par_slot, par_slot, forth)
    s3 = Ship(3, 2 * down + q, 2 * down + q, forth)
    s4 = Ship(4, own_slot, own_slot, back)
    s5 = Ship(5, par_slot, par_slot, back)
    s6 = Ship(6, 2 * up + (1 - q), 2 * up + (1 - q), back)
    load_y.wait()
    for h in range(parts):
        load_x[h].wait()
        for ship in (s0, s1, s4):
            ship.start(h)
    for h in range(parts):
        turn(own_slot, h)

    lane8 = lax.broadcasted_iota(jnp.int32, (8, LANE), 1)
    sub8 = lax.broadcasted_iota(jnp.int32, (8, LANE), 0)

    def pack(p, src):
        n = tiles.count[p]
        for t, tile in enumerate(tiles.part[p]):
            if p == 0:
                gsend_a[t // n, 8 * (t % n):8 * (t % n) + 8, :] = tiles.value(src, tile)
            else:
                gsend_b[8 * t:8 * t + 8, :] = tiles.value(src, tile)

    def adopt(p, src):
        n = tiles.count[p]
        if p == 0:
            held = [src[o].astype(f32) for o in range(side)]
            got = {tile: held[t // n][8 * (t % n):8 * (t % n) + 8] for t, tile in enumerate(tiles.part[p])}
        else:
            got = {tile: src[size_a + 8 * t:size_a + 8 * t + 8, :] for t, tile in enumerate(tiles.part[p])}
        for k in sorted({k for i, k in tiles.part[p] if i is not None}):
            for i in range(0, tiles.nrow, 2):
                v = got[i, k] if i + 1 == tiles.nrow else jnp.concatenate([got[i, k], got[i + 1, k]], axis=0)
                wb[8 * i:8 * i + v.shape[0], k * LANE:(k + 1) * LANE] = v.astype(bf16)
        if (None, 0) in got:
            def left(i):
                return jnp.where(tiles.group() == i % tiles.per, got[None, i // tiles.per], 0.0)
            for i in range(0, tiles.nrow, 2):
                v = left(i) if i + 1 == tiles.nrow else jnp.concatenate([left(i), left(i + 1)], axis=0)
                wb[8 * i:8 * i + v.shape[0], nfull * LANE:] = v.astype(bf16)

    load_w.wait()
    load_m.wait()
    for src, dst in ((1, mom), (0, pos)):
        for p in range(2):
            pack(p, wload.at[src])
        dst[span[0], :] = gsend_a[rpos]
        dst[span[1], :] = gsend_b[0:full_b]
    adopt(0, gsend_a)
    adopt(1, pos)

    def column(ref, dst):
        width = -(-hidden // LANE) * LANE
        v = jnp.concatenate([oload[ref, pl.ds(q, 1), :], jnp.zeros((1, width - hidden), f32)], axis=1)
        lanes = lax.broadcasted_iota(jnp.int32, (8, width), 1)
        subs = lax.broadcasted_iota(jnp.int32, (8, width), 0)
        v = jnp.broadcast_to(v, (8, width))
        for i in range(hs // 8):
            hit = jnp.where(lanes == start + i * 8 + subs, v, 0.0)
            dst[i * 8:(i + 1) * 8, :] = jnp.broadcast_to(jnp.sum(hit, axis=1, keepdims=True), (8, LANE))

    for cp in load_o:
        cp.wait()
    column(0, w2b)
    column(1, m2b)

    rowid = lax.broadcasted_iota(jnp.int32, (hs, LANE), 0)

    split = tiles.lanes

    def hidden_block(par, b, off, first, last, begun=False):
        for n in range(first, last):
            cols = pl.ds(off + n * 256, 256)
            if begun:
                pre = jnp.dot(wb[:, 0:split], xt[0:split, cols], preferred_element_type=f32) + abuf[b, :, n * 256:(n + 1) * 256]
            else:
                pre = jnp.dot(wb[...], xt[:, cols], preferred_element_type=f32)
            act = jnp.tanh(pre)
            abuf[b, :, n * 256:(n + 1) * 256] = act
            for h in range(2):
                part = jnp.sum(act[:, h * LANE:(h + 1) * LANE] * w2z[...], axis=0, keepdims=True)
                zbuf[par, zpos, b, 2 * n + h:2 * n + h + 1, :] = part

    def hidden_start(b, off):
        for n in range(rows // 256):
            abuf[b, :, n * 256:(n + 1) * 256] = jnp.dot(wb[:, split:], xt[split:, pl.ds(off + n * 256, 256)],
                                                        preferred_element_type=f32)

    def first_pass(slot, h):
        per = piece // 256
        hidden_block(0, slot, pl.multiple_of(slot * rows, rows), h * per, (h + 1) * per)

    def take(slot, h):
        turn(slot, h)
        first_pass(slot, h)

    w2z[...] = jnp.where(rowid >= cut, w2b[...], 0.0)
    for h in range(parts):
        s0.landed(h)
        s2.start(h)
        s5.start(h)
    for h in range(parts):
        take(par_slot, h)
        first_pass(own_slot, h)
    for h in range(parts):
        s1.landed(h)
        s3.start(h)
        take(2 * down + q, h)
    for h in range(parts):
        s4.landed(h)
        take(2 * up + q, h)
    for h in range(parts):
        s5.landed(h)
        s6.start(h)
        take(2 * up + (1 - q), h)
    for h in range(parts):
        s2.landed(h)
        take(2 * down + (1 - q), h)
    for h in range(parts):
        s3.landed(h)
        take(2 * far + q, h)
        s6.landed(h)
        take(2 * far + (1 - q), h)

    def z_copy(par, g, d):
        block = pl.ds(blocks[g][0], sizes[g])
        return remote(zbuf.at[par, zpos, block], zbuf.at[par, zpos, block],
                      zsend.at[par, g, d], zrecv.at[par, g, d], zpeer[d])

    def r_copy(p, d, par):
        if p == 0:
            return remote(gsend_a.at[(rpos + d) % side], rsum_a.at[rpos], rsend.at[0, d], rrecv.at[0, d], rpeer[d])
        return remote(gsend_b, rsum_b.at[par, rpos], rsend.at[1 + par, d], rrecv.at[1 + par, d], rpeer[d])

    def a_copy(d):
        return remote(wag_a.at[rpos], wag_a.at[rpos], asend.at[d], arecv.at[d], rpeer[d])

    def fin_ring(arr, d):
        block = fin.at[arr, q, zpos, rpos, 0:head]
        return remote(block, block, fsend.at[arr, d], frecv.at[arr, d], rpeer[d])

    def fin_cross(arr, e, d):
        block = fin.at[arr, q, zpos, (rpos + e) % side, 0:head] if e < side else fin.at[arr, q, zpos, :, head:]
        return remote(block, block, csend.at[arr, e, d], crecv.at[arr, e, d], zpeer[d])

    def fin_pair(arr, w):
        block = fin.at[arr, q, (zpos + w) % side]
        return remote(block, block, psend.at[arr, w], precv.at[arr, w], partner)

    def stage(arr, src, misc):
        fin[arr, q, zpos, rpos, 0:size_a, :] = src[span[0], :]
        fin[arr, q, zpos, rpos, size_a:head, :] = misc
        for r in range(side):
            fin[arr, q, zpos, r, head:, :] = src[size_a + r * size_b:size_a + (r + 1) * size_b, :]

    def spread(arr):
        for d in order:
            fin_ring(arr, d).start()
        for d in order:
            fin_cross(arr, 0, d).start()
        for d in order:
            fin_cross(arr, side, d).start()

    def relay(arr):
        for d in reversed(order):
            fin_ring(arr, d).wait_recv()
            for dd in order:
                fin_cross(arr, side - d, dd).start()

    def over(arr):
        fin_pair(arr, 0).start()
        for w in reversed(order):
            for e in range(side + 1):
                fin_cross(arr, e, side - w).wait_recv()
            fin_pair(arr, w).start()

    for g in range(groups):
        for d in order:
            z_copy(0, g, d).start()
    for ship in (s0, s1, s2, s3, s4, s5, s6):
        ship.sent()

    def squares(main, out):
        low = cut // 8
        sq = jnp.zeros((8, LANE), f32)
        for p in range(2):
            n = tiles.count[p]
            wide = len({k for i, k in tiles.part[p] if i is not None})
            mains = tiles.nrow * wide
            for j in range(n):
                t = n * rpos + j
                at = 8 * j if p == 0 else pl.multiple_of(size_a + 8 * (n * rpos + j), 8)
                v = main[pl.ds(at, 8), :]
                tile_row = jnp.where(t < mains, t // wide + 0 * lane8, (t - mains) * tiles.per + lane8 // rem)
                sq = sq + jnp.where(tile_row >= low, v * v, 0.0)
        for i in range(tiles.nrow):
            v = out[8 * i:8 * i + 8, :]
            sq = sq + jnp.where((i >= low) & (rpos == 0) & (lane8 == 0), v * v, 0.0)
        return sq

    def gradient(k, _):
        par = k % 2

        def weigh(g):
            for d in range(1, side):
                z_copy(par, g, d).wait_recv()
            for b in blocks[g]:
                logit = zbuf[par, 0, b]
                for s in range(1, side):
                    logit = logit + zbuf[par, s, b]
                ztot[b] = logit
                res = ybuf[b].astype(f32) - jax.nn.sigmoid(logit)
                for n in range(nlt):
                    act = abuf[b, :, n * LANE:(n + 1) * LANE]
                    rr = jnp.broadcast_to(res[n:n + 1, :], (hs, LANE))
                    part = rr * act
                    g2acc[...] = part if b == 0 and n == 0 else g2acc[...] + part
                    bbuf[b, :, n * LANE:(n + 1) * LANE] = ((rr * w2b[...]) * (1.0 - act * act)).astype(bf16)

        def contract(g, first, last):
            for lo in range(first, last, 256):
                hi = min(lo + 256, last)
                prod = None
                for b in (range(nshard) if g is None else blocks[g]):
                    one = jnp.dot(bbuf[b], x[b * rows:(b + 1) * rows, lo:hi], preferred_element_type=f32)
                    prod = one if prod is None else prod + one
                gacc[:, lo:hi] = prod if not g else gacc[:, lo:hi] + prod

        for g in range(groups):
            weigh(g)
            contract(g, 0, split)
        pack(0, gacc)
        for d in order:
            r_copy(0, d, par).start()
        g2 = jnp.zeros((8, LANE), f32)
        for i in range(hs // 8):
            col = jnp.sum(g2acc[i * 8:(i + 1) * 8, :], axis=1, keepdims=True)
            g2 = jnp.where(lane8 == i, jnp.broadcast_to(col, (8, LANE)), g2)
        gsend_b[full_b:full_b + 8, :] = g2
        contract(None, split, kpad)
        pack(1, gacc)
        for d in order:
            r_copy(1, d, par).start()
        rsum_a[rpos] = gsend_a[rpos]
        rsum_b[par, rpos] = gsend_b[...]
        for g in range(groups):
            for d in range(1, side):
                z_copy(par, g, d).wait_send()
        coef = jnp.where((k == 0) | (k == LEAPS), 0.5 * step, step).astype(f32)

        def kick(p):
            for d in range(1, side):
                r_copy(p, d, par).wait_recv()
            held = [rsum_a[s] if p == 0 else rsum_b[par, s] for s in range(side)]
            total = held[0]
            for s in range(1, side):
                total = total + held[s]
            size = size_a if p == 0 else full_b
            mom[span[p], :] = mom[span[p], :] + coef * (total[0:size] - pos[span[p], :] / PRIOR_VAR)
            if p == 1:
                g2sum[...] = total[size:size + 8]

        def kick_out():
            tile = g2sum[...]
            for i in range(hs // 8):
                blk = slice(i * 8, (i + 1) * 8)
                gcol = jnp.broadcast_to(tile[:, i:i + 1], (8, LANE))
                m2b[blk, :] = m2b[blk, :] + coef * (gcol - w2b[blk, :] / PRIOR_VAR)

        @pl.when(k < LEAPS)
        def _():
            kick(0)
            pos[span[0], :] = pos[span[0], :] + step * mom[span[0], :]
            wag_a[rpos] = pos[span[0], :].astype(bf16)
            for d in order:
                a_copy(d).start()
            kick(1)
            pos[span[1], :] = pos[span[1], :] + step * mom[span[1], :]
            adopt(1, pos)
            for b in range(begin):
                hidden_start(b, b * rows)
            kick_out()
            w2b[...] = w2b[...] + step * m2b[...]
            w2z[...] = jnp.where(rowid >= cut, w2b[...], 0.0)

            @pl.when(k == LEAPS - 1)
            def _():
                stage(0, pos, jnp.zeros((8, LANE), f32))
                spread(0)

            for p in range(2):
                for d in range(1, side):
                    r_copy(p, d, par).wait_send()
            for d in range(1, side):
                a_copy(d).wait_recv()
            adopt(0, wag_a)
            for g in range(groups):
                for b in blocks[g]:
                    hidden_block(1 - par, b, b * rows, 0, rows // 256, b < begin)
                for d in order:
                    z_copy(1 - par, g, d).start()
            for d in range(1, side):
                a_copy(d).wait_send()

            @pl.when(k == LEAPS - 1)
            def _():
                relay(0)

        @pl.when(k == LEAPS)
        def _():
            loss = jnp.zeros((8, LANE), f32)
            for b in range(nshard):
                zt = ztot[b]
                loss = loss + (jnp.maximum(zt, 0.0) + jnp.log1p(jnp.exp(-jnp.abs(zt))) - ybuf[b].astype(f32) * zt)
            estage[...] = jnp.where(zpos == 0, loss, 0.0) + squares(pos, w2b) / (2.0 * PRIOR_VAR)
            for p in range(2):
                kick(p)
            kick_out()
            for p in range(2):
                for d in range(1, side):
                    r_copy(p, d, par).wait_send()

        return 0

    lax.fori_loop(0, LEAPS + 1, gradient, 0)

    def as_row(ref):
        diag = jnp.where(rowid == lax.broadcasted_iota(jnp.int32, (hs, LANE), 1), ref[...], 0.0)
        return jnp.broadcast_to(jnp.sum(diag, axis=0, keepdims=True), (8, LANE))

    share = jnp.sum(estage[...] + 0.5 * squares(mom, m2b), axis=0, keepdims=True)
    misc = jnp.where(sub8 == 0, as_row(w2b), jnp.where(sub8 == 1, as_row(m2b), jnp.broadcast_to(share, (8, LANE))))

    stage(1, mom, misc)
    spread(1)
    over(0)
    relay(1)
    over(1)
    for arr in range(2):
        for w in range(side):
            fin_pair(arr, w).wait()
        for d in order:
            fin_ring(arr, d).wait_send()
            for e in range(side + 1):
                fin_cross(arr, e, d).wait_send()


def _unpack(cfg, fin, end_w, end_m, w_out, m_out, e_out, obuf, w_row, m_row, energy, sem, tail):
    side, hidden, feat, rows, hs, step, sizes = cfg
    chains = fin.shape[1]
    tiles = Tiles(side, feat, hs)
    base = (0, tiles.size[0] + 8)
    extra = tiles.size[0]
    f32 = jnp.float32
    width = -(-hidden // LANE) * LANE
    lane = lax.broadcasted_iota(jnp.int32, (8, width), 1)
    for ch in range(chains):
        acc = jnp.zeros((8, width), f32)
        tot = jnp.zeros((8, LANE), f32)
        for z in range(side):
            tile = fin[1, ch, z, 0, extra:extra + 8, :]
            wide = jnp.concatenate([tile, jnp.zeros((8, width - LANE), f32)], axis=1)
            r0 = min(z * hs, hidden - hs)
            wide = pltpu.roll(wide, r0, 1) if r0 else wide
            acc = jnp.where((lane >= z * hs) & (lane < (z + 1) * hs), wide, acc)
            for r in range(side):
                tot = tot + fin[1, ch, z, r, extra:extra + 8, :]
        w_row[ch:ch + 1, :] = acc[0:1, 0:hidden]
        m_row[ch:ch + 1, :] = acc[1:2, 0:hidden]
        energy[ch] = jnp.sum(tot[2:3, :])
    copies = [pltpu.make_async_copy(src, dst, tail.at[i]) for i, (src, dst) in enumerate(((w_row, w_out), (m_row, m_out), (energy, e_out)))]
    for cp in copies:
        cp.start()
    for arr, ref in ((0, end_w), (1, end_m)):
        for ch in range(chains):
            for z in range(side):
                r0 = min(z * hs, hidden - hs)
                for p in range(2):
                    n = tiles.count[p]
                    for t, (i, k) in enumerate(tiles.part[p]):
                        at = base[p] + 8 * (t % n)
                        tile = fin[arr, ch, z, t // n, at:at + 8, :]
                        if i is not None:
                            obuf[arr, ch, r0 + 8 * i:r0 + 8 * i + 8, k * LANE:(k + 1) * LANE] = tile
                            continue
                        for g in range(min(tiles.per, tiles.nrow - k * tiles.per)):
                            r1 = r0 + 8 * (k * tiles.per + g)
                            v = pltpu.roll(tile, LANE - g * tiles.rem, 1) if g else tile
                            obuf[arr, ch, r1:r1 + 8, tiles.nfull * LANE:feat] = v[:, 0:tiles.rem]
            cp = pltpu.make_async_copy(obuf.at[arr, ch], ref.at[ch], sem.at[arr, ch])
            cp.start()
            copies.append(cp)
    for cp in copies:
        cp.wait()


def solution(mesh):
    row_spec = P('data', None)
    label_spec = P('data')
    in_spec = P(None, 'parts', None)
    out_spec = P('parts', None)
    chain_spec = P('parts')
    side = math.isqrt(mesh.shape['data'] // 2)

    def run_chains(feats, labels, w_in, w_out, mom_in, mom_out):
        num_rows, feat = feats.shape
        hidden = w_in.shape[2]
        step = 1.0 / math.sqrt(num_rows * (feat + hidden))

        def device_body(x_rows, y_rows, pos_in, pos_out, vel_in, vel_out):
            rows = x_rows.shape[0]
            chains = pos_out.shape[0]
            hs = -(-(hidden // 8) // side) * 8
            kpad = -(-feat // LANE) * LANE
            nshard = 2 * side
            size_a, size_b = Tiles(side, feat, hs).size
            urows = size_a + size_b
            sizes = (3, 3, 2)
            pieces = 4
            groups = len(sizes)
            f32, bf16 = jnp.float32, jnp.bfloat16
            dma = pltpu.SemaphoreType.DMA
            vm = pltpu.VMEM
            cfg = (side, hidden, feat, rows, hs, step, sizes)
            full = jax.ShapeDtypeStruct((chains, hidden, feat), f32)
            any_spec = pl.BlockSpec(memory_space=pl.ANY)
            vmem_spec = pl.BlockSpec(memory_space=pltpu.VMEM)
            hbm_spec = pl.BlockSpec(memory_space=pltpu.HBM)
            piece_shape = (2, chains, side, side, urows + 8, LANE)
            fin = pl.pallas_call(
                functools.partial(_kernel, cfg),
                out_shape=vm(piece_shape, f32),
                in_specs=[hbm_spec] * 6,
                out_specs=vmem_spec,
                scratch_shapes=[
                    vm((kpad, nshard * rows), bf16),
                    vm((nshard * rows, kpad), bf16),
                    vm((nshard, 8, rows // 8), jnp.int32),
                    vm((2, chains, hidden), f32),
                    vm((8, LANE), f32),
                    vm((8, LANE), f32),
                    vm((2, hs, feat), f32),
                    vm((hs, kpad), bf16),
                    vm((nshard, hs, rows), f32),
                    vm((nshard, hs, rows), bf16),
                    vm((hs, kpad), f32),
                    vm((hs, LANE), f32),
                    vm((side, size_a, LANE), f32),
                    vm((side * size_b + 8, LANE), f32),
                    vm((side, size_a, LANE), f32),
                    vm((2, side, side * size_b + 8, LANE), f32),
                    vm((size_a + side * size_b, LANE), f32),
                    vm((size_a + side * size_b, LANE), f32),
                    vm((hs, LANE), f32),
                    vm((hs, LANE), f32),
                    vm((hs, LANE), f32),
                    vm((side, size_a, LANE), bf16),
                    vm((2, side, nshard, 8, LANE), f32),
                    vm((nshard, 8, LANE), f32),
                    dma((2 + pieces,)), dma((7, pieces)), dma((7, pieces)), dma((8,)), dma((9,)),
                    dma((2, groups, side)), dma((2, groups, side)),
                    dma((3, side)), dma((3, side)), dma((side,)), dma((side,)),
                    dma((2, side)), dma((2, side)), dma((2, side + 1, side)), dma((2, side + 1, side)),
                    dma((2, side)), dma((2, side)),
                ],
                compiler_params=pltpu.CompilerParams(collective_id=0, has_side_effects=True, vmem_limit_bytes=67043328 - 4 * math.prod(piece_shape)),
            )(x_rows.T, y_rows.reshape(8, rows // 8), pos_in.transpose(1, 2, 0), vel_in.transpose(1, 2, 0), pos_out, vel_out)
            end_w, end_m, w_row, m_row, energy = pl.pallas_call(
                functools.partial(_unpack, cfg),
                out_shape=(full, full, jax.ShapeDtypeStruct((chains, hidden), f32), jax.ShapeDtypeStruct((chains, hidden), f32),
                           jax.ShapeDtypeStruct((chains,), f32)),
                in_specs=[vmem_spec],
                out_specs=(any_spec,) * 5,
                scratch_shapes=[vm((2, chains, hidden, feat), f32), vm((chains, hidden), f32), vm((chains, hidden), f32),
                                pltpu.SMEM((chains,), f32), dma((2, chains)), dma((3,))],
                compiler_params=pltpu.CompilerParams(vmem_limit_bytes=16 << 20),
            )(fin)
            return end_w.transpose(2, 0, 1), w_row, end_m.transpose(2, 0, 1), m_row, energy

        mapped = jax.shard_map(device_body, mesh=mesh, in_specs=(row_spec, label_spec, in_spec, out_spec, in_spec, out_spec), out_specs=(in_spec, out_spec, in_spec, out_spec, chain_spec), check_vma=False)
        return mapped(feats, labels, w_in, w_out, mom_in, mom_out)

    return run_chains
```

```python
import functools
import math

import jax
import jax.numpy as jnp
from jax import lax
from jax.experimental import pallas as pl
from jax.experimental.pallas import tpu as pltpu
from jax.sharding import PartitionSpec as P

LEAPS = 16
PRIOR_VAR = 1.0
LANE = 128
BEGIN = 6
MESH_ID = pl.DeviceIdType.MESH


class Tiles:
    def __init__(self, side, feat, hs):
        self.nrow = hs // 8
        self.nfull = feat // LANE
        self.rem = feat - self.nfull * LANE
        self.per = LANE // self.rem
        split = 2 * (self.nfull // 3)
        self.lanes = split * LANE
        left = [(None, j) for j in range(-(-self.nrow // self.per))]
        self.part = [[(i, k) for i in range(self.nrow) for k in range(split)],
                     [(i, k) for i in range(self.nrow) for k in range(split, self.nfull)] + left]
        self.count = [len(p) // side for p in self.part]
        assert all(len(p) % side == 0 for p in self.part)
        self.size = [8 * n for n in self.count]

    def value(self, src, tile):
        i, k = tile
        if i is not None:
            return src[8 * i:8 * i + 8, k * LANE:(k + 1) * LANE]
        acc = None
        for g in range(min(self.per, self.nrow - k * self.per)):
            i = k * self.per + g
            v = src[8 * i:8 * i + 8, self.nfull * LANE:src.shape[1]]
            if v.shape[1] < LANE:
                v = jnp.concatenate([v, jnp.zeros((8, LANE - v.shape[1]), v.dtype)], axis=1)
                v = pltpu.roll(v, g * self.rem, 1) if g else v
            else:
                v = jnp.where(self.group() == g, v, 0.0)
            acc = v if acc is None else acc + v
        return acc

    def group(self):
        return lax.broadcasted_iota(jnp.int32, (8, LANE), 1) // self.rem


def _kernel(cfg, xt_hbm, lab_hbm, w_hbm, m_hbm, wo_hbm, mo_hbm, fin,
            xt, x, ybuf, oload, estage, g2sum, wload, wb, abuf, bbuf, gacc, g2acc, gsend_a, gsend_b, rsum_a, rsum_b, pos, mom, w2b, m2b, w2z,
            wag_a, zbuf, ztot,
            lsem, isend, irecv, ysend, yrecv, zsend, zrecv, rsend, rrecv, asend, arecv, fsend, frecv,
            csend, crecv, psend, precv):
    side, hidden, feat, rows, hs, step, sizes = cfg
    half = side // 2
    nshard = 2 * side
    tiles = Tiles(side, feat, hs)
    nfull, rem = tiles.nfull, tiles.rem
    size_a, size_b = tiles.size
    urows = size_a + size_b
    full_b = side * size_b
    head = size_a + 8
    span = (slice(0, size_a), slice(size_a, size_a + full_b))
    kpad = xt.shape[0]
    nlt = rows // LANE
    begin = BEGIN
    groups = len(sizes)
    blocks = [range(sum(sizes[:g]), sum(sizes[:g + 1])) for g in range(groups)]
    f32, bf16 = jnp.float32, jnp.bfloat16

    me = lax.axis_index('data')
    core = me % 2
    xx = (me // 2) % side
    yy = me // (2 * side)

    def fold(y, x_):
        return (x_ // half + y // half) % 2

    q = (core + fold(yy, xx)) % 2
    zpos = xx * (1 - q) + yy * q
    rpos = yy * (1 - q) + xx * q

    def device(z, r, role):
        x2 = z * (1 - role) + r * role
        y2 = r * (1 - role) + z * role
        return {'data': (y2 * side + x2) * 2 + (role + fold(y2, x2)) % 2}

    zpeer = [device((zpos + d) % side, rpos, q) for d in range(side)]
    rpeer = [device(zpos, (rpos + d) % side, q) for d in range(side)]
    partner = device(rpos, zpos, 1 - q)

    def remote(src, dst, ssem, rsem, dev):
        return pltpu.make_async_remote_copy(src_ref=src, dst_ref=dst, send_sem=ssem, recv_sem=rsem,
                                            device_id=dev, device_id_type=MESH_ID)

    start = jnp.minimum(zpos * hs, hidden - hs)
    start = pl.multiple_of(start, 8)
    cut = zpos * hs - start

    own_slot = 2 * zpos + q
    par_slot = 2 * zpos + (1 - q)

    parts = isend.shape[1]
    piece = rows // parts
    order = [d for d in range(1, side) if d == half] + [d for d in range(1, side) if d != half]

    def xcols(slot, h):
        return xt.at[pl.ds(0, feat), pl.ds(pl.multiple_of(slot * rows + h * piece, piece), piece)]

    load_x = [pltpu.make_async_copy(xt_hbm.at[:, pl.ds(h * piece, piece)], xcols(own_slot, h), lsem.at[2 + h]) for h in range(parts)]
    load_w = pltpu.make_async_copy(w_hbm.at[q, pl.ds(start, hs), :], wload.at[0], lsem.at[0])
    load_m = pltpu.make_async_copy(m_hbm.at[q, pl.ds(start, hs), :], wload.at[1], lsem.at[1])
    load_y = pltpu.make_async_copy(lab_hbm, ybuf.at[own_slot], ysend.at[7])
    load_o = [pltpu.make_async_copy(src, oload.at[i], yrecv.at[7 + i]) for i, src in enumerate((wo_hbm, mo_hbm))]
    for cp in load_x + [load_y, load_w, load_m] + load_o:
        cp.start()

    barrier = pltpu.get_barrier_semaphore()
    for dev in zpeer[1:] + rpeer[1:] + [partner]:
        pl.semaphore_signal(barrier, inc=1, device_id=dev, device_id_type=MESH_ID)
    pl.semaphore_wait(barrier, 2 * side - 1)

    class Ship:
        def __init__(self, i, slot, dslot, dev):
            self.x = [remote(xcols(slot, h), xcols(dslot, h), isend.at[i, h], irecv.at[i, h], dev) for h in range(parts)]
            self.y = remote(ybuf.at[slot], ybuf.at[dslot], ysend.at[i], yrecv.at[i], dev)

        def start(self, h):
            self.x[h].start()
            if h == parts - 1:
                self.y.start()

        def landed(self, h):
            self.x[h].wait_recv()
            if h == parts - 1:
                self.y.wait_recv()

        def sent(self):
            for c in self.x:
                c.wait_send()
            self.y.wait_send()

    def turn(slot, h):
        def body(t, _):
            off = pl.multiple_of(slot * rows + h * piece + t * LANE, LANE)
            for row in range(feat, kpad, rem):
                xt[row:row + rem, pl.ds(off, LANE)] = xt[feat - rem:feat, pl.ds(off, LANE)]
            x[pl.ds(off, LANE), :] = xt[:, pl.ds(off, LANE)].T
            return 0
        lax.fori_loop(0, piece // LANE, body, 0)

    up, down, far = (zpos + 1) % side, (zpos + side - 1) % side, (zpos + 2) % side
    forth, back = zpeer[1], zpeer[side - 1]
    s0 = Ship(0, own_slot, 2 * rpos + q, partner)
    s1 = Ship(1, own_slot, own_slot, forth)
    s2 = Ship(2, par_slot, par_slot, forth)
    s3 = Ship(3, 2 * down + q, 2 * down + q, forth)
    s4 = Ship(4, own_slot, own_slot, back)
    s5 = Ship(5, par_slot, par_slot, back)
    s6 = Ship(6, 2 * up + (1 - q), 2 * up + (1 - q), back)
    load_y.wait()
    for h in range(parts):
        load_x[h].wait()
        for ship in (s0, s1, s4):
            ship.start(h)
    for h in range(parts):
        turn(own_slot, h)

    lane8 = lax.broadcasted_iota(jnp.int32, (8, LANE), 1)
    sub8 = lax.broadcasted_iota(jnp.int32, (8, LANE), 0)

    def pack(p, src):
        n = tiles.count[p]
        for t, tile in enumerate(tiles.part[p]):
            if p == 0:
                gsend_a[t // n, 8 * (t % n):8 * (t % n) + 8, :] = tiles.value(src, tile)
            else:
                gsend_b[8 * t:8 * t + 8, :] = tiles.value(src, tile)

    def adopt(p, src):
        n = tiles.count[p]
        if p == 0:
            held = [src[o].astype(f32) for o in range(side)]
            got = {tile: held[t // n][8 * (t % n):8 * (t % n) + 8] for t, tile in enumerate(tiles.part[p])}
        else:
            got = {tile: src[size_a + 8 * t:size_a + 8 * t + 8, :] for t, tile in enumerate(tiles.part[p])}
        for k in sorted({k for i, k in tiles.part[p] if i is not None}):
            for i in range(0, tiles.nrow, 2):
                v = got[i, k] if i + 1 == tiles.nrow else jnp.concatenate([got[i, k], got[i + 1, k]], axis=0)
                wb[8 * i:8 * i + v.shape[0], k * LANE:(k + 1) * LANE] = v.astype(bf16)
        if (None, 0) in got:
            def left(i):
                return jnp.where(tiles.group() == i % tiles.per, got[None, i // tiles.per], 0.0)
            for i in range(0, tiles.nrow, 2):
                v = left(i) if i + 1 == tiles.nrow else jnp.concatenate([left(i), left(i + 1)], axis=0)
                wb[8 * i:8 * i + v.shape[0], nfull * LANE:] = v.astype(bf16)

    load_w.wait()
    load_m.wait()
    for src, dst in ((1, mom), (0, pos)):
        for p in range(2):
            pack(p, wload.at[src])
        dst[span[0], :] = gsend_a[rpos]
        dst[span[1], :] = gsend_b[0:full_b]
    adopt(0, gsend_a)
    adopt(1, pos)

    def column(ref, dst):
        width = -(-hidden // LANE) * LANE
        v = jnp.concatenate([oload[ref, pl.ds(q, 1), :], jnp.zeros((1, width - hidden), f32)], axis=1)
        lanes = lax.broadcasted_iota(jnp.int32, (8, width), 1)
        subs = lax.broadcasted_iota(jnp.int32, (8, width), 0)
        v = jnp.broadcast_to(v, (8, width))
        for i in range(hs // 8):
            hit = jnp.where(lanes == start + i * 8 + subs, v, 0.0)
            dst[i * 8:(i + 1) * 8, :] = jnp.broadcast_to(jnp.sum(hit, axis=1, keepdims=True), (8, LANE))

    for cp in load_o:
        cp.wait()
    column(0, w2b)
    column(1, m2b)

    rowid = lax.broadcasted_iota(jnp.int32, (hs, LANE), 0)

    split = tiles.lanes

    def hidden_block(par, b, off, first, last, begun=False):
        for n in range(first, last):
            cols = pl.ds(off + n * 256, 256)
            if begun:
                pre = jnp.dot(wb[:, 0:split], xt[0:split, cols], preferred_element_type=f32) + abuf[b, :, n * 256:(n + 1) * 256]
            else:
                pre = jnp.dot(wb[...], xt[:, cols], preferred_element_type=f32)
            act = jnp.tanh(pre)
            abuf[b, :, n * 256:(n + 1) * 256] = act
            for h in range(2):
                part = jnp.sum(act[:, h * LANE:(h + 1) * LANE] * w2z[...], axis=0, keepdims=True)
                zbuf[par, zpos, b, 2 * n + h:2 * n + h + 1, :] = part

    def hidden_start(b, off):
        for n in range(rows // 256):
            abuf[b, :, n * 256:(n + 1) * 256] = jnp.dot(wb[:, split:], xt[split:, pl.ds(off + n * 256, 256)],
                                                        preferred_element_type=f32)

    def first_pass(slot, h):
        per = piece // 256
        hidden_block(0, slot, pl.multiple_of(slot * rows, rows), h * per, (h + 1) * per)

    def take(slot, h):
        turn(slot, h)
        first_pass(slot, h)

    w2z[...] = jnp.where(rowid >= cut, w2b[...], 0.0)
    for h in range(parts):
        s0.landed(h)
        s2.start(h)
        s5.start(h)
    for h in range(parts):
        take(par_slot, h)
        first_pass(own_slot, h)
    for h in range(parts):
        s1.landed(h)
        s3.start(h)
        take(2 * down + q, h)
    for h in range(parts):
        s4.landed(h)
        take(2 * up + q, h)
    for h in range(parts):
        s5.landed(h)
        s6.start(h)
        take(2 * up + (1 - q), h)
    for h in range(parts):
        s2.landed(h)
        take(2 * down + (1 - q), h)
    for h in range(parts):
        s3.landed(h)
        take(2 * far + q, h)
        s6.landed(h)
        take(2 * far + (1 - q), h)

    def z_copy(par, g, d):
        block = pl.ds(blocks[g][0], sizes[g])
        return remote(zbuf.at[par, zpos, block], zbuf.at[par, zpos, block],
                      zsend.at[par, g, d], zrecv.at[par, g, d], zpeer[d])

    def r_copy(p, d, par):
        if p == 0:
            return remote(gsend_a.at[(rpos + d) % side], rsum_a.at[rpos], rsend.at[0, d], rrecv.at[0, d], rpeer[d])
        return remote(gsend_b, rsum_b.at[par, rpos], rsend.at[1 + par, d], rrecv.at[1 + par, d], rpeer[d])

    def a_copy(d):
        return remote(wag_a.at[rpos], wag_a.at[rpos], asend.at[d], arecv.at[d], rpeer[d])

    def fin_ring(arr, d):
        block = fin.at[arr, q, zpos, rpos, 0:head]
        return remote(block, block, fsend.at[arr, d], frecv.at[arr, d], rpeer[d])

    def fin_cross(arr, e, d):
        block = fin.at[arr, q, zpos, (rpos + e) % side, 0:head] if e < side else fin.at[arr, q, zpos, :, head:]
        return remote(block, block, csend.at[arr, e, d], crecv.at[arr, e, d], zpeer[d])

    def fin_pair(arr, w, p):
        block = fin.at[arr, q, (zpos + w) % side, :, head:] if p else fin.at[arr, q, (zpos + w) % side, :, 0:head]
        return remote(block, block, psend.at[arr, p, w], precv.at[arr, p, w], partner)

    def stage(arr, src, misc):
        fin[arr, q, zpos, rpos, 0:size_a, :] = src[span[0], :]
        fin[arr, q, zpos, rpos, size_a:head, :] = misc
        for r in range(side):
            fin[arr, q, zpos, r, head:, :] = src[size_a + r * size_b:size_a + (r + 1) * size_b, :]

    def spread(arr):
        for d in order:
            fin_ring(arr, d).start()
        for d in order:
            fin_cross(arr, side, d).start()
        for d in order:
            fin_cross(arr, 0, d).start()

    def relay(arr):
        for d in reversed(order):
            fin_ring(arr, d).wait_recv()
            for dd in order:
                fin_cross(arr, side - d, dd).start()

    def over(arr):
        fin_pair(arr, 0, 1).start()
        fin_pair(arr, 0, 0).start()
        for w in reversed(order):
            fin_cross(arr, side, side - w).wait_recv()
            fin_pair(arr, w, 1).start()
        for w in reversed(order):
            for e in range(side):
                fin_cross(arr, e, side - w).wait_recv()
            fin_pair(arr, w, 0).start()

    for g in range(groups):
        for d in order:
            z_copy(0, g, d).start()
    for ship in (s0, s1, s2, s3, s4, s5, s6):
        ship.sent()

    def squares(main, out):
        low = cut // 8
        sq = jnp.zeros((8, LANE), f32)
        for p in range(2):
            n = tiles.count[p]
            wide = len({k for i, k in tiles.part[p] if i is not None})
            mains = tiles.nrow * wide
            for j in range(n):
                t = n * rpos + j
                at = 8 * j if p == 0 else pl.multiple_of(size_a + 8 * (n * rpos + j), 8)
                v = main[pl.ds(at, 8), :]
                tile_row = jnp.where(t < mains, t // wide + 0 * lane8, (t - mains) * tiles.per + lane8 // rem)
                sq = sq + jnp.where(tile_row >= low, v * v, 0.0)
        for i in range(tiles.nrow):
            v = out[8 * i:8 * i + 8, :]
            sq = sq + jnp.where((i >= low) & (rpos == 0) & (lane8 == 0), v * v, 0.0)
        return sq

    def gradient(k, _):
        par = k % 2

        def weigh(g):
            for d in range(1, side):
                z_copy(par, g, d).wait_recv()
            for b in blocks[g]:
                logit = zbuf[par, 0, b]
                for s in range(1, side):
                    logit = logit + zbuf[par, s, b]
                ztot[b] = logit
                res = ybuf[b].astype(f32) - jax.nn.sigmoid(logit)
                for n in range(nlt):
                    act = abuf[b, :, n * LANE:(n + 1) * LANE]
                    rr = jnp.broadcast_to(res[n:n + 1, :], (hs, LANE))
                    part = rr * act
                    g2acc[...] = part if b == 0 and n == 0 else g2acc[...] + part
                    bbuf[b, :, n * LANE:(n + 1) * LANE] = ((rr * w2b[...]) * (1.0 - act * act)).astype(bf16)

        def contract(g, first, last):
            for lo in range(first, last, 256):
                hi = min(lo + 256, last)
                prod = None
                for b in (range(nshard) if g is None else blocks[g]):
                    one = jnp.dot(bbuf[b], x[b * rows:(b + 1) * rows, lo:hi], preferred_element_type=f32)
                    prod = one if prod is None else prod + one
                gacc[:, lo:hi] = prod if not g else gacc[:, lo:hi] + prod

        for g in range(groups):
            weigh(g)
            contract(g, 0, split)
        pack(0, gacc)
        for d in order:
            r_copy(0, d, par).start()
        g2 = jnp.zeros((8, LANE), f32)
        for i in range(hs // 8):
            col = jnp.sum(g2acc[i * 8:(i + 1) * 8, :], axis=1, keepdims=True)
            g2 = jnp.where(lane8 == i, jnp.broadcast_to(col, (8, LANE)), g2)
        gsend_b[full_b:full_b + 8, :] = g2
        contract(None, split, kpad)
        pack(1, gacc)
        for d in order:
            r_copy(1, d, par).start()
        rsum_a[rpos] = gsend_a[rpos]
        rsum_b[par, rpos] = gsend_b[...]
        for g in range(groups):
            for d in range(1, side):
                z_copy(par, g, d).wait_send()
        coef = jnp.where((k == 0) | (k == LEAPS), 0.5 * step, step).astype(f32)

        def kick(p):
            for d in range(1, side):
                r_copy(p, d, par).wait_recv()
            held = [rsum_a[s] if p == 0 else rsum_b[par, s] for s in range(side)]
            total = held[0]
            for s in range(1, side):
                total = total + held[s]
            size = size_a if p == 0 else full_b
            mom[span[p], :] = mom[span[p], :] + coef * (total[0:size] - pos[span[p], :] / PRIOR_VAR)
            if p == 1:
                g2sum[...] = total[size:size + 8]

        def kick_out():
            tile = g2sum[...]
            for i in range(hs // 8):
                blk = slice(i * 8, (i + 1) * 8)
                gcol = jnp.broadcast_to(tile[:, i:i + 1], (8, LANE))
                m2b[blk, :] = m2b[blk, :] + coef * (gcol - w2b[blk, :] / PRIOR_VAR)

        @pl.when(k < LEAPS)
        def _():
            kick(0)
            pos[span[0], :] = pos[span[0], :] + step * mom[span[0], :]
            wag_a[rpos] = pos[span[0], :].astype(bf16)
            for d in order:
                a_copy(d).start()
            kick(1)
            pos[span[1], :] = pos[span[1], :] + step * mom[span[1], :]
            adopt(1, pos)
            for b in range(begin):
                hidden_start(b, b * rows)
            kick_out()
            w2b[...] = w2b[...] + step * m2b[...]
            w2z[...] = jnp.where(rowid >= cut, w2b[...], 0.0)

            @pl.when(k == LEAPS - 1)
            def _():
                stage(0, pos, jnp.zeros((8, LANE), f32))
                spread(0)

            for p in range(2):
                for d in range(1, side):
                    r_copy(p, d, par).wait_send()
            for d in range(1, side):
                a_copy(d).wait_recv()
            adopt(0, wag_a)
            for g in range(groups):
                for b in blocks[g]:
                    hidden_block(1 - par, b, b * rows, 0, rows // 256, b < begin)
                for d in order:
                    z_copy(1 - par, g, d).start()
            for d in range(1, side):
                a_copy(d).wait_send()

            @pl.when(k == LEAPS - 1)
            def _():
                relay(0)

        @pl.when(k == LEAPS)
        def _():
            loss = jnp.zeros((8, LANE), f32)
            for b in range(nshard):
                zt = ztot[b]
                loss = loss + (jnp.maximum(zt, 0.0) + jnp.log1p(jnp.exp(-jnp.abs(zt))) - ybuf[b].astype(f32) * zt)
            estage[...] = jnp.where(zpos == 0, loss, 0.0) + squares(pos, w2b) / (2.0 * PRIOR_VAR)
            for p in range(2):
                kick(p)
            kick_out()
            for p in range(2):
                for d in range(1, side):
                    r_copy(p, d, par).wait_send()

        return 0

    lax.fori_loop(0, LEAPS + 1, gradient, 0)

    def as_row(ref):
        diag = jnp.where(rowid == lax.broadcasted_iota(jnp.int32, (hs, LANE), 1), ref[...], 0.0)
        return jnp.broadcast_to(jnp.sum(diag, axis=0, keepdims=True), (8, LANE))

    share = jnp.sum(estage[...] + 0.5 * squares(mom, m2b), axis=0, keepdims=True)
    misc = jnp.where(sub8 == 0, as_row(w2b), jnp.where(sub8 == 1, as_row(m2b), jnp.broadcast_to(share, (8, LANE))))

    stage(1, mom, misc)
    spread(1)
    over(0)
    relay(1)
    over(1)
    for arr in range(2):
        for w in range(side):
            for p in range(2):
                fin_pair(arr, w, p).wait()
        for d in order:
            fin_ring(arr, d).wait_send()
            for e in range(side + 1):
                fin_cross(arr, e, d).wait_send()


def _unpack(cfg, fin, end_w, end_m, w_out, m_out, e_out, obuf, w_row, m_row, energy, sem, tail):
    side, hidden, feat, rows, hs, step, sizes = cfg
    chains = fin.shape[1]
    tiles = Tiles(side, feat, hs)
    base = (0, tiles.size[0] + 8)
    extra = tiles.size[0]
    f32 = jnp.float32
    width = -(-hidden // LANE) * LANE
    lane = lax.broadcasted_iota(jnp.int32, (8, width), 1)
    for ch in range(chains):
        acc = jnp.zeros((8, width), f32)
        tot = jnp.zeros((8, LANE), f32)
        for z in range(side):
            tile = fin[1, ch, z, 0, extra:extra + 8, :]
            wide = jnp.concatenate([tile, jnp.zeros((8, width - LANE), f32)], axis=1)
            r0 = min(z * hs, hidden - hs)
            wide = pltpu.roll(wide, r0, 1) if r0 else wide
            acc = jnp.where((lane >= z * hs) & (lane < (z + 1) * hs), wide, acc)
            for r in range(side):
                tot = tot + fin[1, ch, z, r, extra:extra + 8, :]
        w_row[ch:ch + 1, :] = acc[0:1, 0:hidden]
        m_row[ch:ch + 1, :] = acc[1:2, 0:hidden]
        energy[ch] = jnp.sum(tot[2:3, :])
    copies = [pltpu.make_async_copy(src, dst, tail.at[i]) for i, (src, dst) in enumerate(((w_row, w_out), (m_row, m_out), (energy, e_out)))]
    for cp in copies:
        cp.start()
    for arr, ref in ((0, end_w), (1, end_m)):
        for ch in range(chains):
            for z in range(side):
                r0 = min(z * hs, hidden - hs)
                for p in range(2):
                    n = tiles.count[p]
                    for t, (i, k) in enumerate(tiles.part[p]):
                        at = base[p] + 8 * (t % n)
                        tile = fin[arr, ch, z, t // n, at:at + 8, :]
                        if i is not None:
                            obuf[arr, ch, r0 + 8 * i:r0 + 8 * i + 8, k * LANE:(k + 1) * LANE] = tile
                            continue
                        for g in range(min(tiles.per, tiles.nrow - k * tiles.per)):
                            r1 = r0 + 8 * (k * tiles.per + g)
                            v = pltpu.roll(tile, LANE - g * tiles.rem, 1) if g else tile
                            obuf[arr, ch, r1:r1 + 8, tiles.nfull * LANE:feat] = v[:, 0:tiles.rem]
            cp = pltpu.make_async_copy(obuf.at[arr, ch], ref.at[ch], sem.at[arr, ch])
            cp.start()
            copies.append(cp)
    for cp in copies:
        cp.wait()


def solution(mesh):
    row_spec = P('data', None)
    label_spec = P('data')
    in_spec = P(None, 'parts', None)
    out_spec = P('parts', None)
    chain_spec = P('parts')
    side = math.isqrt(mesh.shape['data'] // 2)

    def run_chains(feats, labels, w_in, w_out, mom_in, mom_out):
        num_rows, feat = feats.shape
        hidden = w_in.shape[2]
        step = 1.0 / math.sqrt(num_rows * (feat + hidden))

        def device_body(x_rows, y_rows, pos_in, pos_out, vel_in, vel_out):
            rows = x_rows.shape[0]
            chains = pos_out.shape[0]
            hs = -(-(hidden // 8) // side) * 8
            kpad = -(-feat // LANE) * LANE
            nshard = 2 * side
            size_a, size_b = Tiles(side, feat, hs).size
            urows = size_a + size_b
            sizes = (3, 3, 2)
            pieces = 4
            groups = len(sizes)
            f32, bf16 = jnp.float32, jnp.bfloat16
            dma = pltpu.SemaphoreType.DMA
            vm = pltpu.VMEM
            cfg = (side, hidden, feat, rows, hs, step, sizes)
            full = jax.ShapeDtypeStruct((chains, hidden, feat), f32)
            any_spec = pl.BlockSpec(memory_space=pl.ANY)
            vmem_spec = pl.BlockSpec(memory_space=pltpu.VMEM)
            hbm_spec = pl.BlockSpec(memory_space=pltpu.HBM)
            piece_shape = (2, chains, side, side, urows + 8, LANE)
            fin = pl.pallas_call(
                functools.partial(_kernel, cfg),
                out_shape=vm(piece_shape, f32),
                in_specs=[hbm_spec] * 6,
                out_specs=vmem_spec,
                scratch_shapes=[
                    vm((kpad, nshard * rows), bf16),
                    vm((nshard * rows, kpad), bf16),
                    vm((nshard, 8, rows // 8), jnp.int32),
                    vm((2, chains, hidden), f32),
                    vm((8, LANE), f32),
                    vm((8, LANE), f32),
                    vm((2, hs, feat), f32),
                    vm((hs, kpad), bf16),
                    vm((nshard, hs, rows), f32),
                    vm((nshard, hs, rows), bf16),
                    vm((hs, kpad), f32),
                    vm((hs, LANE), f32),
                    vm((side, size_a, LANE), f32),
                    vm((side * size_b + 8, LANE), f32),
                    vm((side, size_a, LANE), f32),
                    vm((2, side, side * size_b + 8, LANE), f32),
                    vm((size_a + side * size_b, LANE), f32),
                    vm((size_a + side * size_b, LANE), f32),
                    vm((hs, LANE), f32),
                    vm((hs, LANE), f32),
                    vm((hs, LANE), f32),
                    vm((side, size_a, LANE), bf16),
                    vm((2, side, nshard, 8, LANE), f32),
                    vm((nshard, 8, LANE), f32),
                    dma((2 + pieces,)), dma((7, pieces)), dma((7, pieces)), dma((8,)), dma((9,)),
                    dma((2, groups, side)), dma((2, groups, side)),
                    dma((3, side)), dma((3, side)), dma((side,)), dma((side,)),
                    dma((2, side)), dma((2, side)), dma((2, side + 1, side)), dma((2, side + 1, side)),
                    dma((2, 2, side)), dma((2, 2, side)),
                ],
                compiler_params=pltpu.CompilerParams(collective_id=0, has_side_effects=True, vmem_limit_bytes=67043328 - 4 * math.prod(piece_shape)),
            )(x_rows.T, y_rows.reshape(8, rows // 8), pos_in.transpose(1, 2, 0), vel_in.transpose(1, 2, 0), pos_out, vel_out)
            end_w, end_m, w_row, m_row, energy = pl.pallas_call(
                functools.partial(_unpack, cfg),
                out_shape=(full, full, jax.ShapeDtypeStruct((chains, hidden), f32), jax.ShapeDtypeStruct((chains, hidden), f32),
                           jax.ShapeDtypeStruct((chains,), f32)),
                in_specs=[vmem_spec],
                out_specs=(any_spec,) * 5,
                scratch_shapes=[vm((2, chains, hidden, feat), f32), vm((chains, hidden), f32), vm((chains, hidden), f32),
                                pltpu.SMEM((chains,), f32), dma((2, chains)), dma((3,))],
                compiler_params=pltpu.CompilerParams(vmem_limit_bytes=16 << 20),
            )(fin)
            return end_w.transpose(2, 0, 1), w_row, end_m.transpose(2, 0, 1), m_row, energy

        mapped = jax.shard_map(device_body, mesh=mesh, in_specs=(row_spec, label_spec, in_spec, out_spec, in_spec, out_spec), out_specs=(in_spec, out_spec, in_spec, out_spec, chain_spec), check_vma=False)
        return mapped(feats, labels, w_in, w_out, mom_in, mom_out)

    return run_chains
```
